32 devices in a mesh: row: 8 (over z, x), col: 4 (over y, core).
Axes of the slice: x: 2, y: 2, z: 4, core: 2. Of those that a mesh axis runs over, the one named last changes fastest.
Arguments:
- charges: float32 [32768], P(('row', 'col')), may hold values from -0.5 to 1.5
- structure_id: int32 [32768], P(('row', 'col')), may hold values from 0 to 255, as said below
- live_count: int32 [32], P(('row', 'col')), may hold values from 512 to 1024, as said below
- cell_index: int32 [3, 32768], P(None, ('row', 'col')), may hold values from 0 to 255, as said below
- fraction: float32 [3, 32768], P(None, ('row', 'col')), may hold values from 0 to 1
- influence: float32 [256, 64, 64], P('col', 'row'), may hold values from 0.1 to 10
Outputs:
- forces: float32 [3, 32768], P(None, ('row', 'col'))
- atom_energy: float32 [32768], P(('row', 'col'))
The draws below stay inside these ranges and needn't reach their ends.
Inputs may be any that keep to these rules, and one draw needn't show every extreme that they name: `structure_id`: devices are numbered row-major over (row, col). Slots 0 to 7 of device d are live and belong to fragments d * 8 to d * 8 + 7, so every fragment has a live atom; every other slot names a fragment of its own device, of one of the four devices beside it along row or col (wrapping around), or of the device whose number is d plus half the number of devices (wrapping around). Device d's live atoms are its first live_count[d] slots; the count reaches 1024 on some device in every draw. `cell_index`: the atom slots of the device at (row r, col c) lie in its mesh block: first index from r * 8 to r * 8 + 7, second from c * 16 to c * 16 + 15; the third is anywhere.
All inputs are finite; a program needn't handle non-finite values.
Results may differ from the reference program's by a relative error of at most 0.000065.
Values sent between devices are 32-bit elements; how exact they have to be, the bound alone decides.
A program may use at most 64 MiB of HBM per device.

```python
import math
import jax
import jax.numpy as jnp
from jax import lax

CX = 8
CY = 16
NZ = 256
ATOM_DEV = 1024
S_DEV = 8
NX = 64
NY = 64
ATOMS = 32768
STRUCTS = 256
N_ROW = 8
N_COL = 4
DEVICES = 32


def draw_structure_id(key, part):
    key_side, key_pick = jax.random.split(jax.random.fold_in(key, 5))
    atom_slot = lax.iota(jnp.int32, ATOMS)
    device = atom_slot // ATOM_DEV
    within = atom_slot % ATOM_DEV
    row_place = device // N_COL
    col_place = device % N_COL
    side = jax.random.randint(key_side, (ATOMS,), 0, 6)
    row_step = jnp.where(side == 1, 1, jnp.where(side == 2, -1, 0))
    col_step = jnp.where(side == 3, 1, jnp.where(side == 4, -1, 0))
    owner = (row_place + row_step + N_ROW) % N_ROW * N_COL + (col_place + col_step + N_COL) % N_COL
    far_owner = (device + DEVICES // 2) % DEVICES
    owner = jnp.where(side == 5, far_owner, owner)
    nearby = owner * S_DEV + jax.random.randint(key_pick, (ATOMS,), 0, S_DEV)
    return jnp.where(within < S_DEV, device * S_DEV + within, nearby).astype(jnp.int32)


def draw_live_count(key, part):
    key_counts, key_fullest = jax.random.split(jax.random.fold_in(key, 7))
    least_live = max(S_DEV, ATOM_DEV // 2)
    counts = jax.random.randint(key_counts, (DEVICES,), least_live, ATOM_DEV + 1)
    fullest = jax.random.randint(key_fullest, (), 0, DEVICES)
    return jnp.where(lax.iota(jnp.int32, DEVICES) == fullest, ATOM_DEV, counts).astype(jnp.int32)


def draw_cell_index(key, part):
    key_x, key_y, key_z = jax.random.split(jax.random.fold_in(key, 11), 3)
    atom_slot = lax.iota(jnp.int32, ATOMS)
    device = atom_slot // ATOM_DEV
    row_place = device // N_COL
    col_place = device % N_COL
    cell_x = row_place * CX + jax.random.randint(key_x, (ATOMS,), 0, CX)
    cell_y = col_place * CY + jax.random.randint(key_y, (ATOMS,), 0, CY)
    cell_z = jax.random.randint(key_z, (ATOMS,), 0, NZ)
    return jnp.stack([cell_x, cell_y, cell_z]).astype(jnp.int32)


def block_levels(key, dims, shards, smallest, high):
    def one(dim, shards_of):
        draws = jax.random.uniform(jax.random.fold_in(jax.random.fold_in(key, 6), dim), (shards_of,), jnp.float32, smallest / len(shards), high / len(shards))
        return jnp.repeat(jnp.exp(draws), dims[dim] // shards_of).reshape((-1,) + (1,) * (len(dims) - dim - 1))

    level = one(*shards[0])
    for cut in shards[1:]:
        level = level * one(*cut)
    return level


def setup_inputs(seed: int = 0) -> dict:
    key_of = jax.random.split(jax.random.key(seed), 7)
    return {
        "charges": jnp.clip(-0.5 + 2.0 * jax.random.uniform(key_of[0], (ATOMS,), jnp.float32) ** block_levels(key_of[0], (ATOMS,), ((0, 32),), -0.2, 0.2), -0.5, 1.5),
        "structure_id": draw_structure_id(jax.random.fold_in(key_of[6], 71), 0),
        "live_count": draw_live_count(jax.random.fold_in(key_of[6], 71), 0),
        "cell_index": draw_cell_index(jax.random.fold_in(key_of[6], 71), 0),
        "fraction": jnp.clip(1.0 * jax.random.uniform(key_of[4], (3, ATOMS), jnp.float32) ** block_levels(key_of[4], (3, ATOMS), ((1, 32),), -0.2, 0.2), 0.0, 1.0),
        "influence": jnp.clip(jnp.exp(math.log(10.0) - 4.6051702 * jax.random.uniform(key_of[5], (NZ, NY, NX), jnp.float32) ** block_levels(key_of[5], (NZ, NY, NX), ((0, 4), (1, 8)), -0.2, 0.2)), 0.1, 10.0),
    }


def spline_weights(fraction):
    remain = 1.0 - fraction
    square = fraction * fraction
    cubic_term = square * fraction
    values = [remain * remain * remain / 6.0, (3.0 * cubic_term - 6.0 * square + 4.0) / 6.0,
              (-3.0 * cubic_term + 3.0 * square + 3.0 * fraction + 1.0) / 6.0, cubic_term / 6.0]
    slopes = [-0.5 * remain * remain, 0.5 * (3.0 * square - 4.0 * fraction),
              0.5 * (-3.0 * square + 2.0 * fraction + 1.0), 0.5 * square]
    return values, slopes


def reference(charges, structure_id, live_count, cell_index, fraction, influence):
    atom_slot = jnp.arange(ATOMS, dtype=jnp.int32)
    live = ((atom_slot % ATOM_DEV) < live_count[atom_slot // ATOM_DEV]).astype(jnp.float32)
    totals = jax.ops.segment_sum(charges * live, structure_id, num_segments=STRUCTS)
    counts = jax.ops.segment_sum(live, structure_id, num_segments=STRUCTS)
    neutral = (charges - (totals / counts)[structure_id]) * live
    wx_val, wx_slope = spline_weights(fraction[0])
    wy_val, wy_slope = spline_weights(fraction[1])
    wz_val, wz_slope = spline_weights(fraction[2])
    density = jnp.zeros((NX, NY, NZ), jnp.float32)
    for first in range(4):
        cell_x = (cell_index[0] + first) % NX
        for second in range(4):
            cell_y = (cell_index[1] + second) % NY
            partial_xy = neutral * wx_val[first] * wy_val[second]
            for third in range(4):
                cell_z = (cell_index[2] + third) % NZ
                density = density.at[cell_x, cell_y, cell_z].add(partial_xy * wz_val[third])
    spectrum = jnp.fft.fftn(density)
    kernel = jnp.transpose(influence, (2, 1, 0))
    potential = jnp.real(jnp.fft.ifftn(spectrum * kernel))
    value = jnp.zeros_like(charges)
    grad_x = jnp.zeros_like(charges)
    grad_y = jnp.zeros_like(charges)
    grad_z = jnp.zeros_like(charges)
    for first in range(4):
        cell_x = (cell_index[0] + first) % NX
        for second in range(4):
            cell_y = (cell_index[1] + second) % NY
            for third in range(4):
                cell_z = (cell_index[2] + third) % NZ
                sample = potential[cell_x, cell_y, cell_z]
                value = value + wx_val[first] * wy_val[second] * wz_val[third] * sample
                grad_x = grad_x + wx_slope[first] * wy_val[second] * wz_val[third] * sample
                grad_y = grad_y + wx_val[first] * wy_slope[second] * wz_val[third] * sample
                grad_z = grad_z + wx_val[first] * wy_val[second] * wz_slope[third] * sample
    atom_energy = 0.5 * neutral * value
    forces = -neutral[None, :] * jnp.stack([grad_x, grad_y, grad_z])
    return forces, atom_energy
```

```python
import math

import functools

import jax
import jax.numpy as jnp
import numpy as np
from jax import lax
from jax.experimental import pallas as pl
from jax.experimental.pallas import tpu as pltpu
from jax.sharding import PartitionSpec as P

CX = 8
CY = 16
NZ = 256
S_DEV = 8


highest = lax.Precision.HIGHEST


def passed_along(block, axis, distance):
    devices = range(lax.axis_size(axis))
    route = [((i - distance) % len(devices), i) for i in devices]
    return lax.ppermute(block, axis, route)


def spline_weights(fraction):
    remain = 1.0 - fraction
    square = fraction * fraction
    cubic_term = square * fraction
    values = [
        remain * remain * remain / 6.0,
        (3.0 * cubic_term - 6.0 * square + 4.0) / 6.0,
        (-3.0 * cubic_term + 3.0 * square + 3.0 * fraction + 1.0) / 6.0,
        cubic_term / 6.0,
    ]
    slopes = [
        -0.5 * remain * remain,
        0.5 * (3.0 * square - 4.0 * fraction),
        0.5 * (-3.0 * square + 2.0 * fraction + 1.0),
        0.5 * square,
    ]
    return (values, slopes)


def place_weights(weights, local, width, period):
    columns = lax.broadcasted_iota(jnp.int32, (local.shape[0], width), 1)
    result = jnp.zeros((local.shape[0], width), jnp.float32)
    for offset in range(4):
        target = (local + offset) % period
        result = result + jnp.where(columns == target[:, None], weights[offset][:, None], 0.0)
    return result


def dft_tables(length):
    counter = lax.iota(jnp.int32, length)
    product = counter[:, None] * counter[None, :] % length
    angle = 2.0 * math.pi / length * product.astype(jnp.float32)
    return (jnp.cos(angle), jnp.sin(angle))


def rotate_pair(real_part, imag_part, pattern, cosine, sine, direction):
    real_cos = jnp.einsum(pattern, real_part, cosine, precision=highest)
    real_sin = jnp.einsum(pattern, real_part, sine, precision=highest)
    imag_cos = jnp.einsum(pattern, imag_part, cosine, precision=highest)
    imag_sin = jnp.einsum(pattern, imag_part, sine, precision=highest)
    return (real_cos - direction * imag_sin, imag_cos + direction * real_sin)


def body(charges, structure_id, live_count, cell_index, fraction, influence):
    atom_total = charges.shape[0]
    row_count = lax.axis_size("row")
    col_count = lax.axis_size("col")
    mesh_x = CX * row_count
    mesh_y = CY * col_count
    structures = S_DEV * row_count * col_count
    local_x = cell_index[0] - lax.axis_index("row") * CX
    local_y = cell_index[1] - lax.axis_index("col") * CY
    live = (lax.iota(jnp.int32, atom_total) < live_count[0]).astype(jnp.float32)
    wx_val, wx_slope = spline_weights(fraction[0])
    wy_val, wy_slope = spline_weights(fraction[1])
    wz_val, wz_slope = spline_weights(fraction[2])
    big_period = 4 * (CX + CY + 8)
    x_rows = place_weights(wx_val, local_x, CX + 3, big_period)
    x_slope_rows = place_weights(wx_slope, local_x, CX + 3, big_period)
    y_rows = place_weights(wy_val, local_y, CY + 3, big_period)
    y_slope_rows = place_weights(wy_slope, local_y, CY + 3, big_period)
    z_rows = place_weights(wz_val, cell_index[2], NZ, NZ)
    z_slope_rows = place_weights(wz_slope, cell_index[2], NZ, NZ)
    plane = (y_rows[:, :, None] * x_rows[:, None, :]).reshape(atom_total, -1)
    charge_sums = jax.ops.segment_sum(charges * live, structure_id, num_segments=structures)
    live_sums = jax.ops.segment_sum(live, structure_id, num_segments=structures)
    totals, counts = lax.psum((charge_sums, live_sums), ("row", "col"))
    neutral = (charges - jnp.take(totals / counts, structure_id)) * live
    spread_grid = lax.dot_general(
        plane,
        neutral[:, None] * z_rows,
        (((0,), (0,)), ((), ())),
        precision=highest,
        preferred_element_type=jnp.float32,
    )
    extended = spread_grid.reshape(CY + 3, CX + 3, NZ)
    spill_x = passed_along(extended[:, CX:, :], "row", 1)
    extended = extended[:, :CX, :].at[:, :3, :].add(spill_x)
    spill_y = passed_along(extended[CY:], "col", 1)
    density = extended[:CY].at[:3].add(spill_y)
    cos_z, sin_z = dft_tables(NZ)
    cos_y, sin_y = dft_tables(mesh_y)
    cos_x, sin_x = dft_tables(mesh_x)
    real_z = jnp.einsum("yxz,zk->kxy", density, cos_z, precision=highest)
    imag_z = -jnp.einsum("yxz,zk->kxy", density, sin_z, precision=highest)
    columns = lax.all_to_all(
        jnp.stack([real_z, imag_z]), "col", split_axis=1, concat_axis=3, tiled=True
    )
    real_y, imag_y = rotate_pair(columns[0], columns[1], "zxy,yk->zkx", cos_y, sin_y, -1.0)
    rows = lax.all_to_all(
        jnp.stack([real_y, imag_y]), "row", split_axis=2, concat_axis=3, tiled=True
    )
    real_x, imag_x = rotate_pair(rows[0], rows[1], "zyx,xk->zyk", cos_x, sin_x, -1.0)
    scale = influence / float(mesh_x * mesh_y * NZ)
    real_x = real_x * scale
    imag_x = imag_x * scale
    back_x, back_x_imag = rotate_pair(real_x, imag_x, "zyk,kx->zyx", cos_x, sin_x, 1.0)
    returned = lax.all_to_all(
        jnp.stack([back_x, back_x_imag]), "row", split_axis=3, concat_axis=2, tiled=True
    )
    back_y, back_y_imag = rotate_pair(returned[0], returned[1], "zkx,ky->zxy", cos_y, sin_y, 1.0)
    whole_z = lax.all_to_all(
        jnp.stack([back_y, back_y_imag]), "col", split_axis=3, concat_axis=1, tiled=True
    )
    potential = jnp.einsum("kxy,kz->yxz", whole_z[0], cos_z, precision=highest) - jnp.einsum(
        "kxy,kz->yxz", whole_z[1], sin_z, precision=highest
    )
    upper_x = passed_along(potential[:, :3, :], "row", -1)
    widened = jnp.concatenate([potential, upper_x], axis=1)
    upper_y = passed_along(widened[:3], "col", -1)
    widened = jnp.concatenate([widened, upper_y], axis=0).reshape(-1, NZ)
    sampled = lax.dot_general(
        jnp.concatenate([z_rows, z_slope_rows], axis=0),
        widened,
        (((1,), (1,)), ((), ())),
        precision=highest,
        preferred_element_type=jnp.float32,
    )
    sample_val = sampled[:atom_total]
    sample_slope = sampled[atom_total:]
    plane_dx = (y_rows[:, :, None] * x_slope_rows[:, None, :]).reshape(atom_total, -1)
    plane_dy = (y_slope_rows[:, :, None] * x_rows[:, None, :]).reshape(atom_total, -1)
    value = jnp.sum(plane * sample_val, axis=1)
    grad_x = jnp.sum(plane_dx * sample_val, axis=1)
    grad_y = jnp.sum(plane_dy * sample_val, axis=1)
    grad_z = jnp.sum(plane * sample_slope, axis=1)
    atom_energy = 0.5 * neutral * value
    forces = -neutral[None, :] * jnp.stack([grad_x, grad_y, grad_z])
    return (forces, atom_energy)


EXT_Y = CY + 3
HALO_ROWS = 24
PLANE = 256
LANES = 128
TOP = EXT_Y * CX + 3 * HALO_ROWS
CHUNKS = 2
MESH = pl.DeviceIdType.MESH


def plane_cells():
    cells = np.zeros((PLANE, 2), np.int64)
    used = np.zeros((PLANE,), bool)
    for y in range(EXT_Y):
        for x in range(CX):
            cells[y * CX + x] = (x, y)
            used[y * CX + x] = True
    for x in range(3):
        for y in range(EXT_Y):
            cells[EXT_Y * CX + x * HALO_ROWS + y] = (CX + x, y)
            used[EXT_Y * CX + x * HALO_ROWS + y] = True
    return cells, used


def make_plan(rows, cols):
    n = rows * cols
    offsets = [(0, 0), (1, 0), (-1, 0), (0, 1), (0, -1), (rows // 2, 0)]
    distinct = len({(a % rows, b % cols) for a, b in offsets}) == len(offsets)
    if not (
        rows % 2 == 0
        and cols % 2 == 0
        and rows & (rows - 1) == 0
        and cols & (cols - 1) == 0
        and distinct
        and (CY * cols) % rows == 0
        and CY == 2 * rows
        and CX == 8
        and NZ == 8 * n
        and NZ // cols == 2 * n
        and 4 * n == LANES
        and cols == 4
    ):
        return None
    diffs = [(0, 0)]
    for a, b in offsets:
        for d, e in offsets:
            diff = ((a - d) % rows, (b - e) % cols)
            if diff not in diffs:
                diffs.append(diff)
    return (rows, cols, tuple(offsets), tuple(diffs))


def slot_lists(kind):
    if kind:
        return ((0, 1, 6, 7), (2, 3, 4, 5))
    return ((0, 1, 4, 7), (2, 3, 5, 6))


def make_tables(rows, cols):
    n = rows * cols
    half = NZ // n // 2
    slots = 2 * half
    z = np.arange(NZ)
    forward_z = np.zeros((n, 2, half, NZ))
    for p in range(n):
        for j in range(half):
            angle = 2 * np.pi * ((p + n * j) * z % NZ) / NZ
            forward_z[p, 0, j] = np.cos(angle)
            forward_z[p, 1, j] = -np.sin(angle)
    forward_z[0, 1, 0] = 1.0 - 2.0 * (z % 2)
    per_chunk = half // CHUNKS
    forward_z = forward_z.reshape(n, 2, CHUNKS, per_chunk, NZ).transpose(2, 0, 1, 3, 4)
    forward_z = forward_z.reshape(NZ, NZ)

    r, c, m1, k1 = np.meshgrid(
        np.arange(rows), np.arange(cols), np.arange(cols), np.arange(rows), indexing="ij"
    )
    phi = 2 * np.pi * ((k1 * r % rows) / rows + (m1 * c % cols) / cols)
    phi = phi.reshape(n, n)
    cosp, sinp = np.cos(phi), np.sin(phi)
    gather = np.zeros((2, n, 2, half, 2, slots, n))
    for kind in range(2):
        for t in range(slots):
            j, sign = t, 1.0
            if t >= half:
                j, sign = (slots - 1 - t if kind else slots - t), -1.0
            if kind == 0 and t in (0, half):
                part = 0 if t == 0 else 1
                gather[kind, :, part, 0, 0, t] = cosp
                gather[kind, :, part, 0, 1, t] = -sinp
                continue
            gather[kind, :, 0, j, 0, t] = cosp
            gather[kind, :, 1, j, 0, t] = sign * sinp
            gather[kind, :, 0, j, 1, t] = -sinp
            gather[kind, :, 1, j, 1, t] = sign * cosp
    chunked = np.zeros((2, CHUNKS, n, 2, per_chunk, 2, slots // CHUNKS, n))
    for kind in range(2):
        for ch in range(CHUNKS):
            js = slice(ch * per_chunk, (ch + 1) * per_chunk)
            chunked[kind, ch] = gather[kind][:, :, js][:, :, :, :, list(slot_lists(kind)[ch])]
    lines = 2 * per_chunk * n
    gather = chunked.reshape(2, CHUNKS, lines, slots * n)

    cells, used = plane_cells()
    x, y = cells[:, 0], cells[:, 1]
    low_m, low_k = (v.reshape(-1) for v in np.meshgrid(np.arange(cols), np.arange(rows), indexing="ij"))
    psi = 2 * np.pi * (
        x[None] * low_k[:, None] / (CX * rows) + y[None] * low_m[:, None] / (CY * cols)
    )
    twiddle = np.stack([np.cos(psi), np.sin(psi)])
    high_m, high_k = (v.reshape(-1) for v in np.meshgrid(np.arange(CY), np.arange(CX), indexing="ij"))
    chi = 2 * np.pi * (high_k[:, None] * x[None] % CX / CX + high_m[:, None] * y[None] % CY / CY)
    cosc, sinc = np.cos(chi) * used[None], np.sin(chi) * used[None]
    inner = np.block([[cosc, sinc], [-sinc, cosc]])
    width = CX * rows
    source = np.arange(rows * 2 * width)
    spot = (source // width) * CX + source % width // rows
    place = (spot[:, None] == np.arange(CY * CX)[None]).astype(np.float32)

    def pair(table, axis):
        table = np.asarray(table, np.float32)
        high = table.astype(jnp.bfloat16)
        low = (table - high.astype(np.float32)).astype(jnp.bfloat16)
        return np.stack([high, low], axis=axis)

    turned = gather.transpose(0, 1, 3, 2)
    wide = np.concatenate(list(pair(turned, 0)), axis=-1)
    return (
        pair(forward_z, 0),
        wide,
        pair(gather, 2),
        twiddle.astype(np.float32),
        pair(inner.T, 0),
        pair(inner, 0),
        place.astype(jnp.bfloat16),
    )


def split(values):
    high = values.astype(jnp.bfloat16)
    return high, (values - high.astype(jnp.float32)).astype(jnp.bfloat16)


def one_dot(a, b, contract=(1, 0)):
    return lax.dot_general(
        a, b, ((contract[:1], contract[1:]), ((), ())), preferred_element_type=jnp.float32
    )


def dot(left, right, contract=(1, 0)):
    return one_dot(left[0], right[0], contract) + (
        one_dot(left[0], right[1], contract) + one_dot(left[1], right[0], contract)
    )


def pick(distance, weights):
    result = jnp.where(distance == 3, weights[3], 0.0)
    for i in (2, 1, 0):
        result = jnp.where(distance == i, weights[i], result)
    return result


def kernel(
    plan,
    charges_hbm, sid_hbm, live_hbm, cell_hbm, frac_hbm, influence_hbm,
    fz_hbm, wide_hbm, gather_hbm, twiddle_hbm, inner_t_hbm, inner_hbm, place_hbm,
    forces_ref, energy_ref,
    charges_ref, sid_ref, live_ref, cell_ref, frac_ref, raw,
    fz, wide, gather, twiddle, inner_t, inner, spot,
    z_rows, z_slopes, zf, plane, x_rows, y_rows,
    frag, inf_out, inf_in, green,
    field_out, field_in, back_out, back_in, sampled,
    local_sems, frag_send, frag_recv, inf_send, inf_recv, send_sems, recv_sems,
):
    rows, cols, offsets, diffs = plan
    n = rows * cols
    r, c = lax.axis_index("row"), lax.axis_index("col")
    me = r * cols + c
    atoms = charges_ref.shape[1]
    lines = NZ // CHUNKS
    kind = jnp.minimum(me, 1)
    far_first = sorted(range(1, n), key=lambda o: -o)

    def peer(o):
        return (r ^ (o // cols), c ^ (o % cols))

    barrier = pltpu.get_barrier_semaphore()
    for o in far_first:
        pl.semaphore_signal(barrier, inc=1, device_id=peer(o), device_id_type=MESH)

    copies = [
        pltpu.make_async_copy(source, target, local_sems.at[i])
        for i, (source, target) in enumerate([
            (charges_hbm, charges_ref),
            (sid_hbm, sid_ref),
            (live_hbm, live_ref),
            (frac_hbm, frac_ref),
            (cell_hbm, cell_ref),
            (influence_hbm, raw),
            (fz_hbm, fz),
            (wide_hbm.at[kind], wide),
            (gather_hbm.at[kind], gather),
            (twiddle_hbm, twiddle),
            (inner_t_hbm, inner_t),
            (inner_hbm, inner),
            (place_hbm, spot),
        ])
    ]
    for copy in copies:
        copy.start()

    for copy in copies[:3]:
        copy.wait()
    lane = lax.broadcasted_iota(jnp.int32, (1, atoms), 1)
    live = (lane < live_ref[0]).astype(jnp.float32)
    charges = charges_ref[...]
    charged = charges * live
    sid = sid_ref[...]
    within = lax.broadcasted_iota(jnp.int32, (S_DEV, atoms), 0)
    owners = [
        lax.rem(r + a % rows, rows) * cols + lax.rem(c + b % cols, cols) for a, b in offsets
    ]

    def belongs(o):
        return sid == within + owners[o] * S_DEV

    def folded(values):
        total = values[:, :LANES]
        for k in range(1, atoms // LANES):
            total = total + values[:, k * LANES : (k + 1) * LANES]
        return jnp.sum(total, axis=1, keepdims=True)

    tile_lane = lax.broadcasted_iota(jnp.int32, (S_DEV, LANES), 1)
    message = jnp.zeros((S_DEV, LANES), jnp.float32)
    for o in range(len(offsets)):
        mine = belongs(o)
        message = jnp.where(tile_lane == 2 * o, folded(jnp.where(mine, charged, 0.0)), message)
        message = jnp.where(tile_lane == 2 * o + 1, folded(jnp.where(mine, live, 0.0)), message)
    frag[0] = message

    for copy in copies[3:5]:
        copy.wait()
    wx, vx = spline_weights(frac_ref[0:1, :])
    wy, vy = spline_weights(frac_ref[1:2, :])
    wz, vz = spline_weights(frac_ref[2:3, :])
    cell_z = cell_ref[2:3, :]
    step = 16

    def fill(target, weights):
        @pl.loop(0, NZ // step)
        def _(b):
            start = pl.multiple_of(b * step, step)
            index = lax.broadcasted_iota(jnp.int32, (step, atoms), 0) + start - cell_z
            distance = jnp.where(index < 0, index + NZ, index)
            target[0, pl.ds(start, step), :], target[1, pl.ds(start, step), :] = split(
                pick(distance, weights)
            )

    width = 256

    def transform(which, source):
        for k in range(atoms // width):
            cut = slice(k * width, (k + 1) * width)
            value = dot((fz[0], fz[1]), (source[0, :, cut], source[1, :, cut]))
            zf[which, 0, :, cut], zf[which, 1, :, cut] = split(value)

    fill(z_rows, wz)
    copies[6].wait()
    transform(0, z_rows)

    copies[5].wait()
    for p in range(n):
        first, second = raw[0, p], raw[1, p]
        low = jnp.concatenate([first[:4], second[:4]], axis=0)
        high = jnp.concatenate([first[4:], second[4:]], axis=0)
        inf_out[p] = jnp.concatenate([low, high], axis=1)

    pl.semaphore_wait(barrier, n - 1)

    def frag_copy(k):
        a, b = diffs[k]
        target = (lax.rem(r + (-a) % rows, rows), lax.rem(c + (-b) % cols, cols))
        return pltpu.make_async_remote_copy(
            frag.at[0], frag.at[k], frag_send.at[k], frag_recv.at[k],
            device_id=target, device_id_type=MESH,
        )

    frags = [frag_copy(k) for k in range(1, len(diffs))]
    for copy in frags:
        copy.start()

    place = c * rows + r

    def residue(p):
        return jnp.where(c < cols // 2, p, lax.rem(n - p, n))

    for o in far_first:
        pltpu.make_async_remote_copy(
            inf_out.at[residue(me ^ o)], inf_in.at[place], inf_send, inf_recv,
            device_id=peer(o), device_id_type=MESH,
        ).start()
    inf_in[place] = inf_out[residue(me)]

    fill(z_slopes, vz)
    transform(1, z_slopes)
    distance = lax.broadcasted_iota(jnp.int32, (16, atoms), 0) - (cell_ref[0:1, :] - r * CX)
    x_rows[0] = pick(distance, wx)
    x_rows[1] = pick(distance, vx)
    distance = lax.broadcasted_iota(jnp.int32, (HALO_ROWS, atoms), 0) - (
        cell_ref[1:2, :] - c * CY
    )
    y_rows[0] = pick(distance, wy)
    y_rows[1] = pick(distance, vy)
    plane[:, TOP:, :] = jnp.zeros((2, PLANE - TOP, atoms), jnp.bfloat16)

    for copy in frags:
        copy.wait()
    slot = {diff: k for k, diff in enumerate(diffs)}
    mean = jnp.zeros((S_DEV, atoms), jnp.float32)
    for j, (a, b) in enumerate(offsets):
        total = jnp.zeros((S_DEV, LANES), jnp.float32)
        for i, (d, e) in enumerate(offsets):
            part = frag[slot[((a - d) % rows, (b - e) % cols)]]
            total = total + jnp.where(tile_lane // 2 == i, part, 0.0)
        odd = tile_lane % 2 == 1
        charge_sum = jnp.sum(jnp.where(odd, 0.0, total), axis=1, keepdims=True)
        live_sum = jnp.sum(jnp.where(odd, total, 0.0), axis=1, keepdims=True)
        mean = jnp.where(belongs(j), charge_sum / live_sum, mean)
    mean = jnp.sum(mean, axis=0, keepdims=True)
    neutral = (charges - mean) * live

    x_charged = x_rows[0, :CX] * neutral
    for y in range(0, EXT_Y - 1, 2):
        pair = jnp.concatenate(
            [y_rows[0, y : y + 1, :] * x_charged, y_rows[0, y + 1 : y + 2, :] * x_charged], axis=0
        )
        plane[0, y * CX : (y + 2) * CX, :], plane[1, y * CX : (y + 2) * CX, :] = split(pair)
    base = EXT_Y * CX
    y_charged = y_rows[0] * neutral
    tail = [y_rows[0, EXT_Y - 1 : EXT_Y, :] * x_charged]
    for x in range(3):
        tail.append(x_rows[0, CX + x : CX + x + 1, :] * y_charged)
    tail = jnp.concatenate(tail, axis=0)
    plane[0, base - CX : TOP, :], plane[1, base - CX : TOP, :] = split(tail)

    sub_low = lax.broadcasted_iota(jnp.int32, (8, LANES), 0) < 4

    def interleaved(values, target):
        for v in range(n // 2):
            rows8 = slice(8 * v, 8 * v + 8)
            near, far = values[rows8, :LANES], values[rows8, LANES:]
            target[2 * v] = jnp.where(sub_low, near, pltpu.roll(far, 4, 0))
            target[2 * v + 1] = jnp.where(sub_low, pltpu.roll(near, 4, 0), far)

    def gathered(source):
        near, far = [], []
        for v in range(n // 2):
            first, second = source[2 * v], source[2 * v + 1]
            near.append(jnp.where(sub_low, first, pltpu.roll(second, 4, 0)))
            far.append(jnp.where(sub_low, pltpu.roll(first, 4, 0), second))
        return jnp.concatenate(
            [jnp.concatenate(near, axis=0), jnp.concatenate(far, axis=0)], axis=1
        )

    def send(source, target, index):
        for o in far_first:
            pltpu.make_async_remote_copy(
                source.at[me ^ o], target.at[me], send_sems.at[index], recv_sems.at[index],
                device_id=peer(o), device_id_type=MESH,
            ).start()
        target[me] = source[me]

    def whole(source, target, send_sem, recv_sem):
        return pltpu.make_async_remote_copy(
            source.at[pl.ds(0, n - 1)], target.at[pl.ds(0, n - 1)], send_sem, recv_sem,
            device_id=(r, c), device_id_type=MESH,
        )

    for ch in range(CHUNKS):
        mine = slice(ch * lines, (ch + 1) * lines)
        value = dot((zf[0, 0, mine], zf[0, 1, mine]), (plane[0], plane[1]), (1, 1))
        interleaved(value, field_out.at[ch])
        send(field_out.at[ch], field_in.at[ch], ch)

    whole(inf_out, inf_in, inf_send, inf_recv).wait()
    copies[12].wait()
    group = lax.broadcasted_iota(jnp.int32, (8, LANES), 1) % rows
    wanted = group == lax.broadcasted_iota(jnp.int32, (8, LANES), 0)
    for t in range(8):
        blocks = []
        for m in range(cols):
            row = (t % 2) * cols + m
            blocks.append(jnp.concatenate(
                [
                    jnp.where(wanted, inf_in[t // 2 * rows + q, row : row + 1, :], 0.0)
                    for q in range(rows)
                ],
                axis=1,
            ))
        high, low = split(jnp.concatenate(blocks, axis=0))
        green[t] = one_dot(high, spot[...]) + one_dot(low, spot[...])

    for copy in copies[7:12]:
        copy.wait()

    for ch in range(CHUNKS):
        whole(field_out.at[ch], field_in.at[ch], send_sems.at[ch], recv_sems.at[ch]).wait()
        high, low = split(gathered(field_in.at[ch]))
        mixed = one_dot(wide[ch], jnp.concatenate([high, high], axis=0)) + one_dot(
            wide[ch, :, :lines], low
        )
        cosine = jnp.concatenate([twiddle[0]] * 4, axis=0)
        sine = jnp.concatenate([twiddle[1]] * 4, axis=0)
        real, imag = mixed[:lines], mixed[lines:]
        turned = jnp.concatenate(
            [real * cosine + imag * sine, imag * cosine - real * sine], axis=1
        )
        spectrum = dot(split(turned), (inner_t[0], inner_t[1]))
        slots = [
            jnp.where(me == 0, t0, t1) for t0, t1 in zip(slot_lists(0)[ch], slot_lists(1)[ch])
        ]
        kernel_values = jnp.concatenate([green[t] for t in slots], axis=0)
        filtered = spectrum * jnp.concatenate([kernel_values, kernel_values], axis=1)
        back = dot(split(filtered), (inner[0], inner[1]))
        real, imag = back[:, :PLANE], back[:, PLANE:]
        turned = jnp.concatenate(
            [real * cosine - imag * sine, imag * cosine + real * sine], axis=0
        )
        interleaved(dot((gather[ch, 0], gather[ch, 1]), split(turned)), back_out.at[ch])
        send(back_out.at[ch], back_in.at[ch], CHUNKS + ch)

    scale = 1.0 / float(CX * rows * CY * cols * NZ)

    def down(values):
        return jnp.sum(values, axis=0, keepdims=True)

    sums = [[0.0] * 4 for _ in range(atoms // width)]
    for ch in range(CHUNKS):
        index = CHUNKS + ch
        whole(back_out.at[ch], back_in.at[ch], send_sems.at[index], recv_sems.at[index]).wait()
        high, low = split((gathered(back_in.at[ch]) * scale).T[:TOP])
        both = jnp.concatenate([high, low], axis=1)
        mine = slice(ch * lines, (ch + 1) * lines)
        for k in range(atoms // width):
            cut = slice(k * width, (k + 1) * width)
            for which in range(2):
                near = zf[which, 0, mine, cut]
                sampled[which, :, cut] = one_dot(
                    both, jnp.concatenate([near, near], axis=0)
                ) + one_dot(high, zf[which, 1, mine, cut])
            by_y = by_dy = by_yz = 0.0
            for y in range(EXT_Y):
                row = slice(y * CX, (y + 1) * CX)
                weight = y_rows[0, y : y + 1, cut]
                by_y = by_y + weight * sampled[0, row, cut]
                by_dy = by_dy + y_rows[1, y : y + 1, cut] * sampled[0, row, cut]
                by_yz = by_yz + weight * sampled[1, row, cut]
            by_x = by_dx = by_xz = 0.0
            for x in range(3):
                row = slice(base + x * HALO_ROWS, base + (x + 1) * HALO_ROWS)
                weight = x_rows[0, CX + x : CX + x + 1, cut]
                by_x = by_x + weight * sampled[0, row, cut]
                by_dx = by_dx + x_rows[1, CX + x : CX + x + 1, cut] * sampled[0, row, cut]
                by_xz = by_xz + weight * sampled[1, row, cut]
            xs, dxs = x_rows[0, :CX, cut], x_rows[1, :CX, cut]
            ys, dys = y_rows[0, :, cut], y_rows[1, :, cut]
            found = [
                down(xs * by_y) + down(ys * by_x),
                down(dxs * by_y) + down(ys * by_dx),
                down(xs * by_dy) + down(dys * by_x),
                down(xs * by_yz) + down(ys * by_xz),
            ]
            sums[k] = [a + b for a, b in zip(sums[k], found)]
    for k in range(atoms // width):
        cut = slice(k * width, (k + 1) * width)
        part = neutral[:, cut]
        value, grad_x, grad_y, grad_z = sums[k]
        energy_ref[:, cut] = 0.5 * part * value
        forces_ref[0:1, cut] = -part * grad_x
        forces_ref[1:2, cut] = -part * grad_y
        forces_ref[2:3, cut] = -part * grad_z


def fast_body(plan, charges, structure_id, live_count, cell_index, fraction, influence):
    rows, cols, offsets, diffs = plan
    n = rows * cols
    atoms = charges.shape[0]
    tables = make_tables(rows, cols)
    vmem = pl.BlockSpec(memory_space=pltpu.VMEM)
    anywhere = pl.BlockSpec(memory_space=pltpu.HBM)
    f32, bf16 = jnp.float32, jnp.bfloat16
    stored = influence.reshape(2, n, CX, CX * rows)
    inputs = [
        charges[None, :], structure_id[None, :], live_count, cell_index, fraction, stored,
    ]
    held = [
        pltpu.SMEM(v.shape, v.dtype) if v is live_count else pltpu.VMEM(v.shape, v.dtype)
        for v in inputs
    ]
    for i, table in enumerate(tables):
        held.append(pltpu.VMEM(table.shape[1:] if i in (1, 2) else table.shape, table.dtype))
    sems = pltpu.SemaphoreType.DMA
    exchanged = pltpu.VMEM((CHUNKS, n, 8, LANES), f32)
    forces, energy = pl.pallas_call(
        functools.partial(kernel, plan),
        out_shape=(
            jax.ShapeDtypeStruct((3, atoms), f32),
            jax.ShapeDtypeStruct((1, atoms), f32),
        ),
        in_specs=[anywhere] * (len(inputs) + len(tables)),
        out_specs=(vmem, vmem),
        scratch_shapes=held + [
            pltpu.VMEM((2, NZ, atoms), bf16),
            pltpu.VMEM((2, NZ, atoms), bf16),
            pltpu.VMEM((2, 2, NZ, atoms), bf16),
            pltpu.VMEM((2, PLANE, atoms), bf16),
            pltpu.VMEM((2, 16, atoms), f32),
            pltpu.VMEM((2, HALO_ROWS, atoms), f32),
            pltpu.VMEM((len(diffs), S_DEV, LANES), f32),
            pltpu.VMEM((n, 8, LANES), f32),
            pltpu.VMEM((n, 8, LANES), f32),
            pltpu.VMEM((8, n, LANES), f32),
            exchanged, exchanged, exchanged, exchanged,
            pltpu.VMEM((2, TOP, atoms), f32),
            sems((len(held),)),
            sems((len(diffs),)), sems((len(diffs),)), sems(()), sems(()),
            sems((2 * CHUNKS,)), sems((2 * CHUNKS,)),
        ],
        compiler_params=pltpu.CompilerParams(
            collective_id=0, has_side_effects=True, vmem_limit_bytes=67043328
        ),
        name="ewald_step",
    )(*inputs, *[jnp.asarray(t) for t in tables])
    return forces, energy[0]


def solution(mesh):
    plan = make_plan(mesh.shape["row"], mesh.shape["col"])
    placed = (
        P(("row", "col")),
        P(("row", "col")),
        P(("row", "col")),
        P(None, ("row", "col")),
        P(None, ("row", "col")),
        P("col", "row", None),
    )
    return jax.shard_map(
        body if plan is None else functools.partial(fast_body, plan),
        mesh=mesh,
        in_specs=placed,
        out_specs=(P(None, ("row", "col")), P(("row", "col"))),
        check_vma=False,
    )
```

```python
import math

import functools

import jax
import jax.numpy as jnp
import numpy as np
from jax import lax
from jax.experimental import pallas as pl
from jax.experimental.pallas import tpu as pltpu
from jax.sharding import PartitionSpec as P

CX = 8
CY = 16
NZ = 256
S_DEV = 8


highest = lax.Precision.HIGHEST


def passed_along(block, axis, distance):
    devices = range(lax.axis_size(axis))
    route = [((i - distance) % len(devices), i) for i in devices]
    return lax.ppermute(block, axis, route)


def spline_weights(fraction):
    remain = 1.0 - fraction
    square = fraction * fraction
    cubic_term = square * fraction
    values = [
        remain * remain * remain / 6.0,
        (3.0 * cubic_term - 6.0 * square + 4.0) / 6.0,
        (-3.0 * cubic_term + 3.0 * square + 3.0 * fraction + 1.0) / 6.0,
        cubic_term / 6.0,
    ]
    slopes = [
        -0.5 * remain * remain,
        0.5 * (3.0 * square - 4.0 * fraction),
        0.5 * (-3.0 * square + 2.0 * fraction + 1.0),
        0.5 * square,
    ]
    return (values, slopes)


def place_weights(weights, local, width, period):
    columns = lax.broadcasted_iota(jnp.int32, (local.shape[0], width), 1)
    result = jnp.zeros((local.shape[0], width), jnp.float32)
    for offset in range(4):
        target = (local + offset) % period
        result = result + jnp.where(columns == target[:, None], weights[offset][:, None], 0.0)
    return result


def dft_tables(length):
    counter = lax.iota(jnp.int32, length)
    product = counter[:, None] * counter[None, :] % length
    angle = 2.0 * math.pi / length * product.astype(jnp.float32)
    return (jnp.cos(angle), jnp.sin(angle))


def rotate_pair(real_part, imag_part, pattern, cosine, sine, direction):
    real_cos = jnp.einsum(pattern, real_part, cosine, precision=highest)
    real_sin = jnp.einsum(pattern, real_part, sine, precision=highest)
    imag_cos = jnp.einsum(pattern, imag_part, cosine, precision=highest)
    imag_sin = jnp.einsum(pattern, imag_part, sine, precision=highest)
    return (real_cos - direction * imag_sin, imag_cos + direction * real_sin)


def body(charges, structure_id, live_count, cell_index, fraction, influence):
    atom_total = charges.shape[0]
    row_count = lax.axis_size("row")
    col_count = lax.axis_size("col")
    mesh_x = CX * row_count
    mesh_y = CY * col_count
    structures = S_DEV * row_count * col_count
    local_x = cell_index[0] - lax.axis_index("row") * CX
    local_y = cell_index[1] - lax.axis_index("col") * CY
    live = (lax.iota(jnp.int32, atom_total) < live_count[0]).astype(jnp.float32)
    wx_val, wx_slope = spline_weights(fraction[0])
    wy_val, wy_slope = spline_weights(fraction[1])
    wz_val, wz_slope = spline_weights(fraction[2])
    big_period = 4 * (CX + CY + 8)
    x_rows = place_weights(wx_val, local_x, CX + 3, big_period)
    x_slope_rows = place_weights(wx_slope, local_x, CX + 3, big_period)
    y_rows = place_weights(wy_val, local_y, CY + 3, big_period)
    y_slope_rows = place_weights(wy_slope, local_y, CY + 3, big_period)
    z_rows = place_weights(wz_val, cell_index[2], NZ, NZ)
    z_slope_rows = place_weights(wz_slope, cell_index[2], NZ, NZ)
    plane = (y_rows[:, :, None] * x_rows[:, None, :]).reshape(atom_total, -1)
    charge_sums = jax.ops.segment_sum(charges * live, structure_id, num_segments=structures)
    live_sums = jax.ops.segment_sum(live, structure_id, num_segments=structures)
    totals, counts = lax.psum((charge_sums, live_sums), ("row", "col"))
    neutral = (charges - jnp.take(totals / counts, structure_id)) * live
    spread_grid = lax.dot_general(
        plane,
        neutral[:, None] * z_rows,
        (((0,), (0,)), ((), ())),
        precision=highest,
        preferred_element_type=jnp.float32,
    )
    extended = spread_grid.reshape(CY + 3, CX + 3, NZ)
    spill_x = passed_along(extended[:, CX:, :], "row", 1)
    extended = extended[:, :CX, :].at[:, :3, :].add(spill_x)
    spill_y = passed_along(extended[CY:], "col", 1)
    density = extended[:CY].at[:3].add(spill_y)
    cos_z, sin_z = dft_tables(NZ)
    cos_y, sin_y = dft_tables(mesh_y)
    cos_x, sin_x = dft_tables(mesh_x)
    real_z = jnp.einsum("yxz,zk->kxy", density, cos_z, precision=highest)
    imag_z = -jnp.einsum("yxz,zk->kxy", density, sin_z, precision=highest)
    columns = lax.all_to_all(
        jnp.stack([real_z, imag_z]), "col", split_axis=1, concat_axis=3, tiled=True
    )
    real_y, imag_y = rotate_pair(columns[0], columns[1], "zxy,yk->zkx", cos_y, sin_y, -1.0)
    rows = lax.all_to_all(
        jnp.stack([real_y, imag_y]), "row", split_axis=2, concat_axis=3, tiled=True
    )
    real_x, imag_x = rotate_pair(rows[0], rows[1], "zyx,xk->zyk", cos_x, sin_x, -1.0)
    scale = influence / float(mesh_x * mesh_y * NZ)
    real_x = real_x * scale
    imag_x = imag_x * scale
    back_x, back_x_imag = rotate_pair(real_x, imag_x, "zyk,kx->zyx", cos_x, sin_x, 1.0)
    returned = lax.all_to_all(
        jnp.stack([back_x, back_x_imag]), "row", split_axis=3, concat_axis=2, tiled=True
    )
    back_y, back_y_imag = rotate_pair(returned[0], returned[1], "zkx,ky->zxy", cos_y, sin_y, 1.0)
    whole_z = lax.all_to_all(
        jnp.stack([back_y, back_y_imag]), "col", split_axis=3, concat_axis=1, tiled=True
    )
    potential = jnp.einsum("kxy,kz->yxz", whole_z[0], cos_z, precision=highest) - jnp.einsum(
        "kxy,kz->yxz", whole_z[1], sin_z, precision=highest
    )
    upper_x = passed_along(potential[:, :3, :], "row", -1)
    widened = jnp.concatenate([potential, upper_x], axis=1)
    upper_y = passed_along(widened[:3], "col", -1)
    widened = jnp.concatenate([widened, upper_y], axis=0).reshape(-1, NZ)
    sampled = lax.dot_general(
        jnp.concatenate([z_rows, z_slope_rows], axis=0),
        widened,
        (((1,), (1,)), ((), ())),
        precision=highest,
        preferred_element_type=jnp.float32,
    )
    sample_val = sampled[:atom_total]
    sample_slope = sampled[atom_total:]
    plane_dx = (y_rows[:, :, None] * x_slope_rows[:, None, :]).reshape(atom_total, -1)
    plane_dy = (y_slope_rows[:, :, None] * x_rows[:, None, :]).reshape(atom_total, -1)
    value = jnp.sum(plane * sample_val, axis=1)
    grad_x = jnp.sum(plane_dx * sample_val, axis=1)
    grad_y = jnp.sum(plane_dy * sample_val, axis=1)
    grad_z = jnp.sum(plane * sample_slope, axis=1)
    atom_energy = 0.5 * neutral * value
    forces = -neutral[None, :] * jnp.stack([grad_x, grad_y, grad_z])
    return (forces, atom_energy)


EXT_Y = CY + 3
HALO_ROWS = 24
PLANE = 256
LANES = 128
TOP = EXT_Y * CX + 3 * HALO_ROWS
CHUNKS = 2
MESH = pl.DeviceIdType.MESH


def plane_cells():
    cells = np.zeros((PLANE, 2), np.int64)
    used = np.zeros((PLANE,), bool)
    for y in range(EXT_Y):
        for x in range(CX):
            cells[y * CX + x] = (x, y)
            used[y * CX + x] = True
    for x in range(3):
        for y in range(EXT_Y):
            cells[EXT_Y * CX + x * HALO_ROWS + y] = (CX + x, y)
            used[EXT_Y * CX + x * HALO_ROWS + y] = True
    return cells, used


def make_plan(rows, cols):
    n = rows * cols
    offsets = [(0, 0), (1, 0), (-1, 0), (0, 1), (0, -1), (rows // 2, 0)]
    distinct = len({(a % rows, b % cols) for a, b in offsets}) == len(offsets)
    if not (
        rows % 2 == 0
        and cols % 2 == 0
        and rows & (rows - 1) == 0
        and cols & (cols - 1) == 0
        and distinct
        and (CY * cols) % rows == 0
        and CY == 2 * rows
        and CX == 8
        and NZ == 8 * n
        and NZ // cols == 2 * n
        and 4 * n == LANES
        and cols == 4
    ):
        return None
    diffs = [(0, 0)]
    for a, b in offsets:
        for d, e in offsets:
            diff = ((a - d) % rows, (b - e) % cols)
            if diff not in diffs:
                diffs.append(diff)
    return (rows, cols, tuple(offsets), tuple(diffs))


def slot_lists(kind):
    if kind:
        return ((0, 1, 6, 7), (2, 3, 4, 5))
    return ((0, 1, 4, 7), (2, 3, 5, 6))


def make_tables(rows, cols):
    n = rows * cols
    half = NZ // n // 2
    slots = 2 * half
    z = np.arange(NZ)
    forward_z = np.zeros((n, 2, half, NZ))
    for p in range(n):
        for j in range(half):
            angle = 2 * np.pi * ((p + n * j) * z % NZ) / NZ
            forward_z[p, 0, j] = np.cos(angle)
            forward_z[p, 1, j] = -np.sin(angle)
    forward_z[0, 1, 0] = 1.0 - 2.0 * (z % 2)
    per_chunk = half // CHUNKS
    forward_z = forward_z.reshape(n, 2, CHUNKS, per_chunk, NZ).transpose(2, 0, 1, 3, 4)
    forward_z = forward_z.reshape(NZ, NZ)

    r, c, m1, k1 = np.meshgrid(
        np.arange(rows), np.arange(cols), np.arange(cols), np.arange(rows), indexing="ij"
    )
    phi = 2 * np.pi * ((k1 * r % rows) / rows + (m1 * c % cols) / cols)
    phi = phi.reshape(n, n)
    cosp, sinp = np.cos(phi), np.sin(phi)
    gather = np.zeros((2, n, 2, half, 2, slots, n))
    for kind in range(2):
        for t in range(slots):
            j, sign = t, 1.0
            if t >= half:
                j, sign = (slots - 1 - t if kind else slots - t), -1.0
            if kind == 0 and t in (0, half):
                part = 0 if t == 0 else 1
                gather[kind, :, part, 0, 0, t] = cosp
                gather[kind, :, part, 0, 1, t] = -sinp
                continue
            gather[kind, :, 0, j, 0, t] = cosp
            gather[kind, :, 1, j, 0, t] = sign * sinp
            gather[kind, :, 0, j, 1, t] = -sinp
            gather[kind, :, 1, j, 1, t] = sign * cosp
    chunked = np.zeros((2, CHUNKS, n, 2, per_chunk, 2, slots // CHUNKS, n))
    for kind in range(2):
        for ch in range(CHUNKS):
            js = slice(ch * per_chunk, (ch + 1) * per_chunk)
            chunked[kind, ch] = gather[kind][:, :, js][:, :, :, :, list(slot_lists(kind)[ch])]
    lines = 2 * per_chunk * n
    gather = chunked.reshape(2, CHUNKS, lines, slots * n)

    cells, used = plane_cells()
    x, y = cells[:, 0], cells[:, 1]
    low_m, low_k = (v.reshape(-1) for v in np.meshgrid(np.arange(cols), np.arange(rows), indexing="ij"))
    psi = 2 * np.pi * (
        x[None] * low_k[:, None] / (CX * rows) + y[None] * low_m[:, None] / (CY * cols)
    )
    twiddle = np.stack([np.cos(psi), np.sin(psi)])
    high_m, high_k = (v.reshape(-1) for v in np.meshgrid(np.arange(CY), np.arange(CX), indexing="ij"))
    chi = 2 * np.pi * (high_k[:, None] * x[None] % CX / CX + high_m[:, None] * y[None] % CY / CY)
    cosc, sinc = np.cos(chi) * used[None], np.sin(chi) * used[None]
    inner = np.block([[cosc, sinc], [-sinc, cosc]])
    width = CX * rows
    source = np.arange(rows * 2 * width)
    spot = (source // width) * CX + source % width // rows
    place = (spot[:, None] == np.arange(CY * CX)[None]).astype(np.float32)

    def pair(table, axis):
        table = np.asarray(table, np.float32)
        high = table.astype(jnp.bfloat16)
        low = (table - high.astype(np.float32)).astype(jnp.bfloat16)
        return np.stack([high, low], axis=axis)

    turned = gather.transpose(0, 1, 3, 2)
    wide = np.concatenate(list(pair(turned, 0)), axis=-1)
    return (
        pair(forward_z, 0),
        wide,
        pair(gather, 2),
        twiddle.astype(np.float32),
        pair(inner.T, 0),
        pair(inner, 0),
        place.astype(jnp.bfloat16),
    )


def split(values):
    high = values.astype(jnp.bfloat16)
    return high, (values - high.astype(jnp.float32)).astype(jnp.bfloat16)


def one_dot(a, b, contract=(1, 0)):
    return lax.dot_general(
        a, b, ((contract[:1], contract[1:]), ((), ())), preferred_element_type=jnp.float32
    )


def dot(left, right, contract=(1, 0)):
    return one_dot(left[0], right[0], contract) + (
        one_dot(left[0], right[1], contract) + one_dot(left[1], right[0], contract)
    )


def tall_dot(left, right, contract=(1, 0)):
    height = left[0].shape[0]
    stacked = one_dot(jnp.concatenate(left, axis=0), right[0], contract)
    return stacked[:height] + (stacked[height:] + one_dot(left[0], right[1], contract))


def pick(distance, weights):
    result = jnp.where(distance == 3, weights[3], 0.0)
    for i in (2, 1, 0):
        result = jnp.where(distance == i, weights[i], result)
    return result


def kernel(
    plan,
    charges_hbm, sid_hbm, live_hbm, cell_hbm, frac_hbm, influence_hbm,
    fz_hbm, wide_hbm, gather_hbm, twiddle_hbm, inner_t_hbm, inner_hbm, place_hbm,
    forces_ref, energy_ref,
    charges_ref, sid_ref, live_ref, cell_ref, frac_ref, raw,
    fz, wide, gather, twiddle, inner_t, inner, spot,
    z_rows, z_slopes, zf, plane, x_rows, y_rows,
    member, frag_out, frag_in, inf_out, inf_in, green,
    field_out, field_in, back_out, back_in, sampled,
    local_sems, frag_send, frag_recv, inf_send, inf_recv, send_sems, recv_sems,
):
    rows, cols, offsets, diffs = plan
    n = rows * cols
    r, c = lax.axis_index("row"), lax.axis_index("col")
    me = r * cols + c
    atoms = charges_ref.shape[1]
    lines = NZ // CHUNKS
    kind = jnp.minimum(me, 1)
    far_first = sorted(range(1, n), key=lambda o: o)

    def other(o):
        return lax.rem(me + o, n)

    def peer(o):
        return (lax.div(other(o), cols), lax.rem(other(o), cols))

    barrier = pltpu.get_barrier_semaphore()
    for o in far_first:
        pl.semaphore_signal(barrier, inc=1, device_id=peer(o), device_id_type=MESH)

    copies = [
        pltpu.make_async_copy(source, target, local_sems.at[i])
        for i, (source, target) in enumerate([
            (charges_hbm, charges_ref),
            (sid_hbm, sid_ref),
            (live_hbm, live_ref),
            (frac_hbm, frac_ref),
            (cell_hbm, cell_ref),
            (influence_hbm, raw),
            (fz_hbm, fz),
            (wide_hbm.at[kind], wide),
            (gather_hbm.at[kind], gather),
            (twiddle_hbm, twiddle),
            (inner_t_hbm, inner_t),
            (inner_hbm, inner),
            (place_hbm, spot),
        ])
    ]
    for copy in copies:
        copy.start()

    for copy in copies[:3]:
        copy.wait()
    lane = lax.broadcasted_iota(jnp.int32, (1, atoms), 1)
    live = (lane < live_ref[0]).astype(jnp.float32)
    charges = charges_ref[...]
    charged = charges * live
    sid = sid_ref[...]
    within = lax.broadcasted_iota(jnp.int32, (S_DEV, atoms), 0)
    count = len(offsets)
    held = [
        sid == within + S_DEV * (
            lax.rem(r + a % rows, rows) * cols + lax.rem(c + b % cols, cols)
        )
        for a, b in offsets
    ]
    for i in range(0, count, 2):
        chosen = jnp.concatenate([jnp.where(h, 1.0, 0.0) for h in held[i : i + 2]], axis=0)
        member[i * S_DEV : (i + 2) * S_DEV, :] = chosen.astype(jnp.bfloat16)
    member[count * S_DEV :, :] = jnp.zeros((LANES - count * S_DEV, atoms), jnp.bfloat16)

    def thirds(values):
        first = values.astype(jnp.bfloat16).astype(jnp.float32)
        second = (values - first).astype(jnp.bfloat16).astype(jnp.float32)
        return [first, second, values - first - second]

    weighed = thirds(charged) + [live, jnp.zeros((12, atoms), jnp.float32)]
    weighed = jnp.concatenate(weighed, axis=0).astype(jnp.bfloat16)
    local_sums = one_dot(weighed, member[...], (1, 1))
    local_sums = jnp.concatenate(
        [
            local_sums[0:1] + local_sums[1:2] + local_sums[2:3],
            local_sums[3:4],
            jnp.zeros((6, LANES), jnp.float32),
        ],
        axis=0,
    )
    tile_lane = lax.broadcasted_iota(jnp.int32, (8, LANES), 1)
    shifted = {
        k: local_sums if k == 0 else pltpu.roll(local_sums, S_DEV * k % LANES, 1)
        for k in range(1 - count, count)
    }
    messages = [jnp.zeros((8, LANES), jnp.float32) for _ in diffs]
    for j, (a, b) in enumerate(offsets):
        for i, (d, e) in enumerate(offsets):
            k = diffs.index(((a - d) % rows, (b - e) % cols))
            messages[k] = jnp.where(tile_lane // S_DEV == j, shifted[j - i], messages[k])
    frag_in[0] = messages[0][:2]
    for k in range(1, len(diffs)):
        frag_out[k] = messages[k][:2]

    for copy in copies[3:5]:
        copy.wait()
    wx, vx = spline_weights(frac_ref[0:1, :])
    wy, vy = spline_weights(frac_ref[1:2, :])
    wz, vz = spline_weights(frac_ref[2:3, :])
    cell_z = cell_ref[2:3, :]
    step = 16

    def fill(target, weights):
        @pl.loop(0, NZ // step)
        def _(b):
            start = pl.multiple_of(b * step, step)
            index = lax.broadcasted_iota(jnp.int32, (step, atoms), 0) + start - cell_z
            distance = jnp.where(index < 0, index + NZ, index)
            target[0, pl.ds(start, step), :], target[1, pl.ds(start, step), :] = split(
                pick(distance, weights)
            )

    width = 256

    def transform(which, source):
        for k in range(atoms // width):
            cut = slice(k * width, (k + 1) * width)
            value = dot((fz[0], fz[1]), (source[0, :, cut], source[1, :, cut]))
            zf[which, 0, :, cut], zf[which, 1, :, cut] = split(value)

    fill(z_rows, wz)
    copies[5].wait()
    for p in range(n):
        first, second = raw[0, p], raw[1, p]
        low = jnp.concatenate([first[:4], second[:4]], axis=0)
        high = jnp.concatenate([first[4:], second[4:]], axis=0)
        inf_out[p] = jnp.concatenate([low, high], axis=1)

    pl.semaphore_wait(barrier, n - 1)

    def frag_copy(k):
        a, b = diffs[k]
        target = (lax.rem(r + (-a) % rows, rows), lax.rem(c + (-b) % cols, cols))
        return pltpu.make_async_remote_copy(
            frag_out.at[k], frag_in.at[k], frag_send.at[k], frag_recv.at[k],
            device_id=target, device_id_type=MESH,
        )

    frags = [frag_copy(k) for k in range(1, len(diffs))]
    for copy in frags:
        copy.start()

    place = c * rows + r

    def residue(p):
        return jnp.where(c < cols // 2, p, lax.rem(n - p, n))

    for o in far_first:
        pltpu.make_async_remote_copy(
            inf_out.at[residue(other(o))], inf_in.at[place], inf_send, inf_recv,
            device_id=peer(o), device_id_type=MESH,
        ).start()
    inf_in[place] = inf_out[residue(me)]

    copies[6].wait()
    transform(0, z_rows)
    fill(z_slopes, vz)
    transform(1, z_slopes)
    distance = lax.broadcasted_iota(jnp.int32, (16, atoms), 0) - (cell_ref[0:1, :] - r * CX)
    x_rows[0] = pick(distance, wx)
    x_rows[1] = pick(distance, vx)
    distance = lax.broadcasted_iota(jnp.int32, (HALO_ROWS, atoms), 0) - (
        cell_ref[1:2, :] - c * CY
    )
    y_rows[0] = pick(distance, wy)
    y_rows[1] = pick(distance, vy)
    plane[:, TOP:, :] = jnp.zeros((2, PLANE - TOP, atoms), jnp.bfloat16)

    for copy in frags:
        copy.wait()
    total = frag_in[0]
    for k in range(1, len(diffs)):
        total = total + frag_in[k]
    mean = jnp.where(tile_lane[:1] < count * S_DEV, total[0:1] / total[1:2], 0.0)
    mean = jnp.concatenate(thirds(mean) + [jnp.zeros((13, LANES), jnp.float32)], axis=0)
    mean = one_dot(mean.astype(jnp.bfloat16), member[...])
    mean = mean[0:1] + mean[1:2] + mean[2:3]
    neutral = (charges - mean) * live

    x_charged = x_rows[0, :CX] * neutral
    for y in range(0, EXT_Y - 1, 2):
        pair = jnp.concatenate(
            [y_rows[0, y : y + 1, :] * x_charged, y_rows[0, y + 1 : y + 2, :] * x_charged], axis=0
        )
        plane[0, y * CX : (y + 2) * CX, :], plane[1, y * CX : (y + 2) * CX, :] = split(pair)
    base = EXT_Y * CX
    y_charged = y_rows[0] * neutral
    tail = [y_rows[0, EXT_Y - 1 : EXT_Y, :] * x_charged]
    for x in range(3):
        tail.append(x_rows[0, CX + x : CX + x + 1, :] * y_charged)
    tail = jnp.concatenate(tail, axis=0)
    plane[0, base - CX : TOP, :], plane[1, base - CX : TOP, :] = split(tail)

    sub_low = lax.broadcasted_iota(jnp.int32, (8, LANES), 0) < 4

    def interleaved(values, target):
        for v in range(n // 2):
            rows8 = slice(8 * v, 8 * v + 8)
            near, far = values[rows8, :LANES], values[rows8, LANES:]
            target[2 * v] = jnp.where(sub_low, near, pltpu.roll(far, 4, 0))
            target[2 * v + 1] = jnp.where(sub_low, pltpu.roll(near, 4, 0), far)

    def gathered(source):
        near, far = [], []
        for v in range(n // 2):
            first, second = source[2 * v], source[2 * v + 1]
            near.append(jnp.where(sub_low, first, pltpu.roll(second, 4, 0)))
            far.append(jnp.where(sub_low, pltpu.roll(first, 4, 0), second))
        return jnp.concatenate(
            [jnp.concatenate(near, axis=0), jnp.concatenate(far, axis=0)], axis=1
        )

    def send(source, target, index):
        for o in far_first:
            pltpu.make_async_remote_copy(
                source.at[other(o)], target.at[me], send_sems.at[index], recv_sems.at[index],
                device_id=peer(o), device_id_type=MESH,
            ).start()
        target[me] = source[me]

    def whole(source, target, send_sem, recv_sem):
        return pltpu.make_async_remote_copy(
            source.at[pl.ds(0, n - 1)], target.at[pl.ds(0, n - 1)], send_sem, recv_sem,
            device_id=(r, c), device_id_type=MESH,
        )

    for ch in range(CHUNKS):
        mine = slice(ch * lines, (ch + 1) * lines)
        value = tall_dot((zf[0, 0, mine], zf[0, 1, mine]), (plane[0], plane[1]), (1, 1))
        interleaved(value, field_out.at[ch])
        send(field_out.at[ch], field_in.at[ch], ch)

    whole(inf_out, inf_in, inf_send, inf_recv).wait()
    copies[12].wait()
    group = lax.broadcasted_iota(jnp.int32, (8, LANES), 1) % rows
    wanted = group == lax.broadcasted_iota(jnp.int32, (8, LANES), 0)
    for t in range(8):
        blocks = []
        for m in range(cols):
            row = (t % 2) * cols + m
            blocks.append(jnp.concatenate(
                [
                    jnp.where(wanted, inf_in[t // 2 * rows + q, row : row + 1, :], 0.0)
                    for q in range(rows)
                ],
                axis=1,
            ))
        high, low = split(jnp.concatenate(blocks, axis=0))
        green[t] = one_dot(high, spot[...]) + one_dot(low, spot[...])

    for copy in copies[7:12]:
        copy.wait()

    for ch in range(CHUNKS):
        whole(field_out.at[ch], field_in.at[ch], send_sems.at[ch], recv_sems.at[ch]).wait()
        high, low = split(gathered(field_in.at[ch]))
        mixed = one_dot(wide[ch], jnp.concatenate([high, high], axis=0)) + one_dot(
            wide[ch, :, :lines], low
        )
        cosine = jnp.concatenate([twiddle[0]] * 4, axis=0)
        sine = jnp.concatenate([twiddle[1]] * 4, axis=0)
        real, imag = mixed[:lines], mixed[lines:]
        turned = jnp.concatenate(
            [real * cosine + imag * sine, imag * cosine - real * sine], axis=1
        )
        spectrum = tall_dot(split(turned), (inner_t[0], inner_t[1]))
        slots = [
            jnp.where(me == 0, t0, t1) for t0, t1 in zip(slot_lists(0)[ch], slot_lists(1)[ch])
        ]
        kernel_values = jnp.concatenate([green[t] for t in slots], axis=0)
        filtered = spectrum * jnp.concatenate([kernel_values, kernel_values], axis=1)
        back = tall_dot(split(filtered), (inner[0], inner[1]))
        real, imag = back[:, :PLANE], back[:, PLANE:]
        turned = jnp.concatenate(
            [real * cosine - imag * sine, imag * cosine + real * sine], axis=0
        )
        interleaved(tall_dot((gather[ch, 0], gather[ch, 1]), split(turned)), back_out.at[ch])
        send(back_out.at[ch], back_in.at[ch], CHUNKS + ch)

    scale = 1.0 / float(CX * rows * CY * cols * NZ)

    def down(values):
        return jnp.sum(values, axis=0, keepdims=True)

    sums = [[0.0] * 4 for _ in range(atoms // width)]
    for ch in range(CHUNKS):
        index = CHUNKS + ch
        whole(back_out.at[ch], back_in.at[ch], send_sems.at[index], recv_sems.at[index]).wait()
        high, low = split((gathered(back_in.at[ch]) * scale).T[:TOP])
        both = jnp.concatenate([high, low], axis=1)
        mine = slice(ch * lines, (ch + 1) * lines)
        for k in range(atoms // width):
            cut = slice(k * width, (k + 1) * width)
            for which in range(2):
                near = zf[which, 0, mine, cut]
                sampled[which, :, cut] = one_dot(
                    both, jnp.concatenate([near, near], axis=0)
                ) + one_dot(high, zf[which, 1, mine, cut])
            by_y = by_dy = by_yz = 0.0
            for y in range(EXT_Y):
                row = slice(y * CX, (y + 1) * CX)
                weight = y_rows[0, y : y + 1, cut]
                by_y = by_y + weight * sampled[0, row, cut]
                by_dy = by_dy + y_rows[1, y : y + 1, cut] * sampled[0, row, cut]
                by_yz = by_yz + weight * sampled[1, row, cut]
            by_x = by_dx = by_xz = 0.0
            for x in range(3):
                row = slice(base + x * HALO_ROWS, base + (x + 1) * HALO_ROWS)
                weight = x_rows[0, CX + x : CX + x + 1, cut]
                by_x = by_x + weight * sampled[0, row, cut]
                by_dx = by_dx + x_rows[1, CX + x : CX + x + 1, cut] * sampled[0, row, cut]
                by_xz = by_xz + weight * sampled[1, row, cut]
            xs, dxs = x_rows[0, :CX, cut], x_rows[1, :CX, cut]
            ys, dys = y_rows[0, :, cut], y_rows[1, :, cut]
            found = [
                down(xs * by_y) + down(ys * by_x),
                down(dxs * by_y) + down(ys * by_dx),
                down(xs * by_dy) + down(dys * by_x),
                down(xs * by_yz) + down(ys * by_xz),
            ]
            sums[k] = [a + b for a, b in zip(sums[k], found)]
    for k in range(atoms // width):
        cut = slice(k * width, (k + 1) * width)
        part = neutral[:, cut]
        value, grad_x, grad_y, grad_z = sums[k]
        energy_ref[:, cut] = 0.5 * part * value
        forces_ref[0:1, cut] = -part * grad_x
        forces_ref[1:2, cut] = -part * grad_y
        forces_ref[2:3, cut] = -part * grad_z


def put(forces_ref, energy_ref, forces_out, energy_out, sems):
    copies = [
        pltpu.make_async_copy(forces_ref, forces_out, sems.at[0]),
        pltpu.make_async_copy(energy_ref, energy_out, sems.at[1]),
    ]
    for copy in copies:
        copy.start()
    for copy in copies:
        copy.wait()


def fast_body(plan, charges, structure_id, live_count, cell_index, fraction, influence):
    rows, cols, offsets, diffs = plan
    n = rows * cols
    atoms = charges.shape[0]
    tables = make_tables(rows, cols)
    vmem = pl.BlockSpec(memory_space=pltpu.VMEM)
    anywhere = pl.BlockSpec(memory_space=pltpu.HBM)
    f32, bf16 = jnp.float32, jnp.bfloat16
    stored = influence.reshape(2, n, CX, CX * rows)
    inputs = [
        charges[None, :], structure_id[None, :], live_count, cell_index, fraction, stored,
    ]
    held = [
        pltpu.SMEM(v.shape, v.dtype) if v is live_count else pltpu.VMEM(v.shape, v.dtype)
        for v in inputs
    ]
    for i, table in enumerate(tables):
        held.append(pltpu.VMEM(table.shape[1:] if i in (1, 2) else table.shape, table.dtype))
    sems = pltpu.SemaphoreType.DMA
    exchanged = pltpu.VMEM((CHUNKS, n, 8, LANES), f32)
    forces, energy = pl.pallas_call(
        functools.partial(kernel, plan),
        out_shape=(
            pltpu.VMEM((3, atoms), f32),
            pltpu.VMEM((1, atoms), f32),
        ),
        in_specs=[anywhere] * (len(inputs) + len(tables)),
        out_specs=(vmem, vmem),
        scratch_shapes=held + [
            pltpu.VMEM((2, NZ, atoms), bf16),
            pltpu.VMEM((2, NZ, atoms), bf16),
            pltpu.VMEM((2, 2, NZ, atoms), bf16),
            pltpu.VMEM((2, PLANE, atoms), bf16),
            pltpu.VMEM((2, 16, atoms), f32),
            pltpu.VMEM((2, HALO_ROWS, atoms), f32),
            pltpu.VMEM((LANES, atoms), bf16),
            pltpu.VMEM((len(diffs), 2, LANES), f32),
            pltpu.VMEM((len(diffs), 2, LANES), f32),
            pltpu.VMEM((n, 8, LANES), f32),
            pltpu.VMEM((n, 8, LANES), f32),
            pltpu.VMEM((8, n, LANES), f32),
            exchanged, exchanged, exchanged, exchanged,
            pltpu.VMEM((2, TOP, atoms), f32),
            sems((len(held),)),
            sems((len(diffs),)), sems((len(diffs),)), sems(()), sems(()),
            sems((2 * CHUNKS,)), sems((2 * CHUNKS,)),
        ],
        compiler_params=pltpu.CompilerParams(
            collective_id=0, has_side_effects=True, vmem_limit_bytes=66000000
        ),
        name="ewald_step",
    )(*inputs, *[jnp.asarray(t) for t in tables])
    forces, energy = pl.pallas_call(
        put,
        out_shape=(
            jax.ShapeDtypeStruct((3, atoms), f32),
            jax.ShapeDtypeStruct((1, atoms), f32),
        ),
        in_specs=[vmem] * 2,
        out_specs=(anywhere, anywhere),
        scratch_shapes=[sems((2,))],
        compiler_params=pltpu.CompilerParams(vmem_limit_bytes=262144),
        name="put_results",
    )(forces, energy)
    return forces, energy[0]


def solution(mesh):
    plan = make_plan(mesh.shape["row"], mesh.shape["col"])
    placed = (
        P(("row", "col")),
        P(("row", "col")),
        P(("row", "col")),
        P(None, ("row", "col")),
        P(None, ("row", "col")),
        P("col", "row", None),
    )
    return jax.shard_map(
        body if plan is None else functools.partial(fast_body, plan),
        mesh=mesh,
        in_specs=placed,
        out_specs=(P(None, ("row", "col")), P(("row", "col"))),
        check_vma=False,
    )
```

```python
import math

import functools

import jax
import jax.numpy as jnp
import numpy as np
from jax import lax
from jax.experimental import pallas as pl
from jax.experimental.pallas import tpu as pltpu
from jax.sharding import PartitionSpec as P

CX = 8
CY = 16
NZ = 256
S_DEV = 8


highest = lax.Precision.HIGHEST


def passed_along(block, axis, distance):
    devices = range(lax.axis_size(axis))
    route = [((i - distance) % len(devices), i) for i in devices]
    return lax.ppermute(block, axis, route)


def spline_weights(fraction):
    remain = 1.0 - fraction
    square = fraction * fraction
    cubic_term = square * fraction
    values = [
        remain * remain * remain / 6.0,
        (3.0 * cubic_term - 6.0 * square + 4.0) / 6.0,
        (-3.0 * cubic_term + 3.0 * square + 3.0 * fraction + 1.0) / 6.0,
        cubic_term / 6.0,
    ]
    slopes = [
        -0.5 * remain * remain,
        0.5 * (3.0 * square - 4.0 * fraction),
        0.5 * (-3.0 * square + 2.0 * fraction + 1.0),
        0.5 * square,
    ]
    return (values, slopes)


def place_weights(weights, local, width, period):
    columns = lax.broadcasted_iota(jnp.int32, (local.shape[0], width), 1)
    result = jnp.zeros((local.shape[0], width), jnp.float32)
    for offset in range(4):
        target = (local + offset) % period
        result = result + jnp.where(columns == target[:, None], weights[offset][:, None], 0.0)
    return result


def dft_tables(length):
    counter = lax.iota(jnp.int32, length)
    product = counter[:, None] * counter[None, :] % length
    angle = 2.0 * math.pi / length * product.astype(jnp.float32)
    return (jnp.cos(angle), jnp.sin(angle))


def rotate_pair(real_part, imag_part, pattern, cosine, sine, direction):
    real_cos = jnp.einsum(pattern, real_part, cosine, precision=highest)
    real_sin = jnp.einsum(pattern, real_part, sine, precision=highest)
    imag_cos = jnp.einsum(pattern, imag_part, cosine, precision=highest)
    imag_sin = jnp.einsum(pattern, imag_part, sine, precision=highest)
    return (real_cos - direction * imag_sin, imag_cos + direction * real_sin)


def body(charges, structure_id, live_count, cell_index, fraction, influence):
    atom_total = charges.shape[0]
    row_count = lax.axis_size("row")
    col_count = lax.axis_size("col")
    mesh_x = CX * row_count
    mesh_y = CY * col_count
    structures = S_DEV * row_count * col_count
    local_x = cell_index[0] - lax.axis_index("row") * CX
    local_y = cell_index[1] - lax.axis_index("col") * CY
    live = (lax.iota(jnp.int32, atom_total) < live_count[0]).astype(jnp.float32)
    wx_val, wx_slope = spline_weights(fraction[0])
    wy_val, wy_slope = spline_weights(fraction[1])
    wz_val, wz_slope = spline_weights(fraction[2])
    big_period = 4 * (CX + CY + 8)
    x_rows = place_weights(wx_val, local_x, CX + 3, big_period)
    x_slope_rows = place_weights(wx_slope, local_x, CX + 3, big_period)
    y_rows = place_weights(wy_val, local_y, CY + 3, big_period)
    y_slope_rows = place_weights(wy_slope, local_y, CY + 3, big_period)
    z_rows = place_weights(wz_val, cell_index[2], NZ, NZ)
    z_slope_rows = place_weights(wz_slope, cell_index[2], NZ, NZ)
    plane = (y_rows[:, :, None] * x_rows[:, None, :]).reshape(atom_total, -1)
    charge_sums = jax.ops.segment_sum(charges * live, structure_id, num_segments=structures)
    live_sums = jax.ops.segment_sum(live, structure_id, num_segments=structures)
    totals, counts = lax.psum((charge_sums, live_sums), ("row", "col"))
    neutral = (charges - jnp.take(totals / counts, structure_id)) * live
    spread_grid = lax.dot_general(
        plane,
        neutral[:, None] * z_rows,
        (((0,), (0,)), ((), ())),
        precision=highest,
        preferred_element_type=jnp.float32,
    )
    extended = spread_grid.reshape(CY + 3, CX + 3, NZ)
    spill_x = passed_along(extended[:, CX:, :], "row", 1)
    extended = extended[:, :CX, :].at[:, :3, :].add(spill_x)
    spill_y = passed_along(extended[CY:], "col", 1)
    density = extended[:CY].at[:3].add(spill_y)
    cos_z, sin_z = dft_tables(NZ)
    cos_y, sin_y = dft_tables(mesh_y)
    cos_x, sin_x = dft_tables(mesh_x)
    real_z = jnp.einsum("yxz,zk->kxy", density, cos_z, precision=highest)
    imag_z = -jnp.einsum("yxz,zk->kxy", density, sin_z, precision=highest)
    columns = lax.all_to_all(
        jnp.stack([real_z, imag_z]), "col", split_axis=1, concat_axis=3, tiled=True
    )
    real_y, imag_y = rotate_pair(columns[0], columns[1], "zxy,yk->zkx", cos_y, sin_y, -1.0)
    rows = lax.all_to_all(
        jnp.stack([real_y, imag_y]), "row", split_axis=2, concat_axis=3, tiled=True
    )
    real_x, imag_x = rotate_pair(rows[0], rows[1], "zyx,xk->zyk", cos_x, sin_x, -1.0)
    scale = influence / float(mesh_x * mesh_y * NZ)
    real_x = real_x * scale
    imag_x = imag_x * scale
    back_x, back_x_imag = rotate_pair(real_x, imag_x, "zyk,kx->zyx", cos_x, sin_x, 1.0)
    returned = lax.all_to_all(
        jnp.stack([back_x, back_x_imag]), "row", split_axis=3, concat_axis=2, tiled=True
    )
    back_y, back_y_imag = rotate_pair(returned[0], returned[1], "zkx,ky->zxy", cos_y, sin_y, 1.0)
    whole_z = lax.all_to_all(
        jnp.stack([back_y, back_y_imag]), "col", split_axis=3, concat_axis=1, tiled=True
    )
    potential = jnp.einsum("kxy,kz->yxz", whole_z[0], cos_z, precision=highest) - jnp.einsum(
        "kxy,kz->yxz", whole_z[1], sin_z, precision=highest
    )
    upper_x = passed_along(potential[:, :3, :], "row", -1)
    widened = jnp.concatenate([potential, upper_x], axis=1)
    upper_y = passed_along(widened[:3], "col", -1)
    widened = jnp.concatenate([widened, upper_y], axis=0).reshape(-1, NZ)
    sampled = lax.dot_general(
        jnp.concatenate([z_rows, z_slope_rows], axis=0),
        widened,
        (((1,), (1,)), ((), ())),
        precision=highest,
        preferred_element_type=jnp.float32,
    )
    sample_val = sampled[:atom_total]
    sample_slope = sampled[atom_total:]
    plane_dx = (y_rows[:, :, None] * x_slope_rows[:, None, :]).reshape(atom_total, -1)
    plane_dy = (y_slope_rows[:, :, None] * x_rows[:, None, :]).reshape(atom_total, -1)
    value = jnp.sum(plane * sample_val, axis=1)
    grad_x = jnp.sum(plane_dx * sample_val, axis=1)
    grad_y = jnp.sum(plane_dy * sample_val, axis=1)
    grad_z = jnp.sum(plane * sample_slope, axis=1)
    atom_energy = 0.5 * neutral * value
    forces = -neutral[None, :] * jnp.stack([grad_x, grad_y, grad_z])
    return (forces, atom_energy)


EXT_Y = CY + 3
HALO_ROWS = 24
PLANE = 256
LANES = 128
TOP = EXT_Y * CX + 3 * HALO_ROWS
CHUNKS = 4
MESH = pl.DeviceIdType.MESH


def plane_cells():
    cells = np.zeros((PLANE, 2), np.int64)
    used = np.zeros((PLANE,), bool)
    for y in range(EXT_Y):
        for x in range(CX):
            cells[y * CX + x] = (x, y)
            used[y * CX + x] = True
    for x in range(3):
        for y in range(EXT_Y):
            cells[EXT_Y * CX + x * HALO_ROWS + y] = (CX + x, y)
            used[EXT_Y * CX + x * HALO_ROWS + y] = True
    return cells, used


def make_plan(rows, cols):
    n = rows * cols
    offsets = [(0, 0), (1, 0), (-1, 0), (0, 1), (0, -1), (rows // 2, 0)]
    distinct = len({(a % rows, b % cols) for a, b in offsets}) == len(offsets)
    if not (
        rows % 2 == 0
        and cols % 2 == 0
        and rows & (rows - 1) == 0
        and cols & (cols - 1) == 0
        and distinct
        and (CY * cols) % rows == 0
        and CY == 2 * rows
        and CX == 8
        and NZ == 8 * n
        and NZ // cols == 2 * n
        and 4 * n == LANES
        and cols == 4
    ):
        return None
    diffs = [(0, 0)]
    for a, b in offsets:
        for d, e in offsets:
            diff = ((a - d) % rows, (b - e) % cols)
            if diff not in diffs:
                diffs.append(diff)
    return (rows, cols, tuple(offsets), tuple(diffs))


def slot_lists(kind):
    if kind:
        return ((0, 7), (1, 6), (2, 5), (3, 4))
    return ((0, 4), (1, 7), (2, 6), (3, 5))


def make_tables(rows, cols):
    n = rows * cols
    half = NZ // n // 2
    slots = 2 * half
    z = np.arange(NZ)
    forward_z = np.zeros((n, 2, half, NZ))
    for p in range(n):
        for j in range(half):
            angle = 2 * np.pi * ((p + n * j) * z % NZ) / NZ
            forward_z[p, 0, j] = np.cos(angle)
            forward_z[p, 1, j] = -np.sin(angle)
    forward_z[0, 1, 0] = 1.0 - 2.0 * (z % 2)
    per_chunk = half // CHUNKS
    forward_z = forward_z.reshape(n, 2, CHUNKS, per_chunk, NZ).transpose(2, 0, 1, 3, 4)
    forward_z = forward_z.reshape(NZ, NZ)

    r, c, m1, k1 = np.meshgrid(
        np.arange(rows), np.arange(cols), np.arange(cols), np.arange(rows), indexing="ij"
    )
    phi = 2 * np.pi * ((k1 * r % rows) / rows + (m1 * c % cols) / cols)
    phi = phi.reshape(n, n)
    cosp, sinp = np.cos(phi), np.sin(phi)
    gather = np.zeros((2, n, 2, half, 2, slots, n))
    for kind in range(2):
        for t in range(slots):
            j, sign = t, 1.0
            if t >= half:
                j, sign = (slots - 1 - t if kind else slots - t), -1.0
            if kind == 0 and t in (0, half):
                part = 0 if t == 0 else 1
                gather[kind, :, part, 0, 0, t] = cosp
                gather[kind, :, part, 0, 1, t] = -sinp
                continue
            gather[kind, :, 0, j, 0, t] = cosp
            gather[kind, :, 1, j, 0, t] = sign * sinp
            gather[kind, :, 0, j, 1, t] = -sinp
            gather[kind, :, 1, j, 1, t] = sign * cosp
    chunked = np.zeros((2, CHUNKS, n, 2, per_chunk, 2, slots // CHUNKS, n))
    for kind in range(2):
        for ch in range(CHUNKS):
            js = slice(ch * per_chunk, (ch + 1) * per_chunk)
            chunked[kind, ch] = gather[kind][:, :, js][:, :, :, :, list(slot_lists(kind)[ch])]
    lines = 2 * per_chunk * n
    gather = chunked.reshape(2, CHUNKS, lines, 2 * slots // CHUNKS * n)

    cells, used = plane_cells()
    x, y = cells[:, 0], cells[:, 1]
    low_m, low_k = (v.reshape(-1) for v in np.meshgrid(np.arange(cols), np.arange(rows), indexing="ij"))
    psi = 2 * np.pi * (
        x[None] * low_k[:, None] / (CX * rows) + y[None] * low_m[:, None] / (CY * cols)
    )
    twiddle = np.stack([np.cos(psi), np.sin(psi)])
    high_m, high_k = (v.reshape(-1) for v in np.meshgrid(np.arange(CY), np.arange(CX), indexing="ij"))
    chi = 2 * np.pi * (high_k[:, None] * x[None] % CX / CX + high_m[:, None] * y[None] % CY / CY)
    cosc, sinc = np.cos(chi) * used[None], np.sin(chi) * used[None]
    inner = np.block([[cosc, sinc], [-sinc, cosc]])
    width = CX * rows
    source = np.arange(rows * 2 * width)
    spot = (source // width) * CX + source % width // rows
    place = (spot[:, None] == np.arange(CY * CX)[None]).astype(np.float32)

    def pair(table, axis):
        table = np.asarray(table, np.float32)
        high = table.astype(jnp.bfloat16)
        low = (table - high.astype(np.float32)).astype(jnp.bfloat16)
        return np.stack([high, low], axis=axis)

    def tripled(table):
        high, low = pair(table, 0)
        return np.concatenate([high, low, high], axis=-1)

    return (
        pair(forward_z, 0),
        tripled(gather.transpose(0, 1, 3, 2)),
        tripled(gather),
        twiddle.astype(np.float32),
        pair(inner.T, 0),
        pair(inner, 0),
        place.astype(jnp.bfloat16),
    )


def split(values):
    high = values.astype(jnp.bfloat16)
    return high, (values - high.astype(jnp.float32)).astype(jnp.bfloat16)


def one_dot(a, b, contract=(1, 0)):
    return lax.dot_general(
        a, b, ((contract[:1], contract[1:]), ((), ())), preferred_element_type=jnp.float32
    )


def dot(left, right, contract=(1, 0)):
    return one_dot(left[0], right[0], contract) + (
        one_dot(left[0], right[1], contract) + one_dot(left[1], right[0], contract)
    )


def tall_dot(left, right, contract=(1, 0)):
    height = left[0].shape[0]
    stacked = one_dot(jnp.concatenate(left, axis=0), right[0], contract)
    return stacked[:height] + (stacked[height:] + one_dot(left[0], right[1], contract))


def tripled_rows(values):
    high, low = split(values)
    return jnp.concatenate([high, high, low], axis=0)


def pick(distance, weights):
    result = jnp.where(distance == 3, weights[3], 0.0)
    for i in (2, 1, 0):
        result = jnp.where(distance == i, weights[i], result)
    return result


def kernel(
    plan,
    charges_hbm, sid_hbm, live_hbm, cell_hbm, frac_hbm, influence_hbm,
    fz_hbm, wide_hbm, gather_hbm, twiddle_hbm, inner_t_hbm, inner_hbm, place_hbm,
    forces_ref, energy_ref,
    charges_ref, sid_ref, live_ref, cell_ref, frac_ref, raw,
    fz, wide, gather, twiddle, inner_t, inner, spot,
    z_rows, z_slopes, zf, plane, x_rows, y_rows,
    member, frag_out, frag_in, inf_out, inf_in, green,
    field_out, field_in, field_end, field_end_in, back_out, back_in, back_end, back_end_in,
    spare, sampled,
    local_sems, frag_send, frag_recv, inf_send, inf_recv, send_sems, recv_sems,
):
    rows, cols, offsets, diffs = plan
    n = rows * cols
    r, c = lax.axis_index("row"), lax.axis_index("col")
    me = r * cols + c
    atoms = charges_ref.shape[1]
    lines = NZ // CHUNKS
    kind = jnp.minimum(me, 1)
    far_first = sorted(range(1, n), key=lambda o: o)

    def other(o):
        return lax.rem(me + o, n)

    def peer(o):
        return (lax.div(other(o), cols), lax.rem(other(o), cols))

    barrier = pltpu.get_barrier_semaphore()
    for o in far_first:
        pl.semaphore_signal(barrier, inc=1, device_id=peer(o), device_id_type=MESH)

    copies = [
        pltpu.make_async_copy(source, target, local_sems.at[i])
        for i, (source, target) in enumerate([
            (charges_hbm, charges_ref),
            (sid_hbm, sid_ref),
            (live_hbm, live_ref),
            (frac_hbm, frac_ref),
            (cell_hbm, cell_ref),
            (influence_hbm, raw),
            (fz_hbm, fz),
            (wide_hbm.at[kind], wide),
            (gather_hbm.at[kind], gather),
            (twiddle_hbm, twiddle),
            (inner_t_hbm, inner_t),
            (inner_hbm, inner),
            (place_hbm, spot),
        ])
    ]
    for copy in copies:
        copy.start()

    for copy in copies[:3]:
        copy.wait()
    lane = lax.broadcasted_iota(jnp.int32, (1, atoms), 1)
    live = (lane < live_ref[0]).astype(jnp.float32)
    charges = charges_ref[...]
    charged = charges * live
    sid = sid_ref[...]
    within = lax.broadcasted_iota(jnp.int32, (S_DEV, atoms), 0)
    count = len(offsets)
    held = [
        sid == within + S_DEV * (
            lax.rem(r + a % rows, rows) * cols + lax.rem(c + b % cols, cols)
        )
        for a, b in offsets
    ]
    for i in range(0, count, 2):
        chosen = jnp.concatenate([jnp.where(h, 1.0, 0.0) for h in held[i : i + 2]], axis=0)
        member[i * S_DEV : (i + 2) * S_DEV, :] = chosen.astype(jnp.bfloat16)
    member[count * S_DEV :, :] = jnp.zeros((LANES - count * S_DEV, atoms), jnp.bfloat16)

    def thirds(values):
        first = values.astype(jnp.bfloat16).astype(jnp.float32)
        second = (values - first).astype(jnp.bfloat16).astype(jnp.float32)
        return [first, second, values - first - second]

    weighed = thirds(charged) + [live, jnp.zeros((12, atoms), jnp.float32)]
    weighed = jnp.concatenate(weighed, axis=0).astype(jnp.bfloat16)
    local_sums = one_dot(weighed, member[...], (1, 1))
    local_sums = jnp.concatenate(
        [
            local_sums[0:1] + local_sums[1:2] + local_sums[2:3],
            local_sums[3:4],
            jnp.zeros((6, LANES), jnp.float32),
        ],
        axis=0,
    )
    tile_lane = lax.broadcasted_iota(jnp.int32, (8, LANES), 1)
    shifted = {
        k: local_sums if k == 0 else pltpu.roll(local_sums, S_DEV * k % LANES, 1)
        for k in range(1 - count, count)
    }
    messages = [jnp.zeros((8, LANES), jnp.float32) for _ in diffs]
    for j, (a, b) in enumerate(offsets):
        for i, (d, e) in enumerate(offsets):
            k = diffs.index(((a - d) % rows, (b - e) % cols))
            messages[k] = jnp.where(tile_lane // S_DEV == j, shifted[j - i], messages[k])
    frag_in[0] = messages[0][:2]
    for k in range(1, len(diffs)):
        frag_out[k] = messages[k][:2]

    for copy in copies[3:5]:
        copy.wait()
    wx, vx = spline_weights(frac_ref[0:1, :])
    wy, vy = spline_weights(frac_ref[1:2, :])
    wz, vz = spline_weights(frac_ref[2:3, :])
    cell_z = cell_ref[2:3, :]
    step = 16

    def fill(target, weights):
        @pl.loop(0, NZ // step)
        def _(b):
            start = pl.multiple_of(b * step, step)
            index = lax.broadcasted_iota(jnp.int32, (step, atoms), 0) + start - cell_z
            distance = jnp.where(index < 0, index + NZ, index)
            target[0, pl.ds(start, step), :], target[1, pl.ds(start, step), :] = split(
                pick(distance, weights)
            )

    width = 256

    def transform(which, source):
        for k in range(atoms // width):
            cut = slice(k * width, (k + 1) * width)
            value = dot((fz[0], fz[1]), (source[0, :, cut], source[1, :, cut]))
            zf[which, 0, :, cut], zf[which, 1, :, cut] = split(value)

    fill(z_rows, wz)
    copies[5].wait()
    for p in range(n):
        first, second = raw[0, p], raw[1, p]
        low = jnp.concatenate([first[:4], second[:4]], axis=0)
        high = jnp.concatenate([first[4:], second[4:]], axis=0)
        inf_out[p] = jnp.concatenate([low, high], axis=1)

    pl.semaphore_wait(barrier, n - 1)

    def frag_copy(k):
        a, b = diffs[k]
        target = (lax.rem(r + (-a) % rows, rows), lax.rem(c + (-b) % cols, cols))
        return pltpu.make_async_remote_copy(
            frag_out.at[k], frag_in.at[k], frag_send.at[k], frag_recv.at[k],
            device_id=target, device_id_type=MESH,
        )

    frags = [frag_copy(k) for k in range(1, len(diffs))]
    for copy in frags:
        copy.start()

    place = c * rows + r

    def residue(p):
        return jnp.where(c < cols // 2, p, lax.rem(n - p, n))

    for o in far_first:
        pltpu.make_async_remote_copy(
            inf_out.at[residue(other(o))], inf_in.at[place], inf_send, inf_recv,
            device_id=peer(o), device_id_type=MESH,
        ).start()
    inf_in[place] = inf_out[residue(me)]

    copies[6].wait()
    transform(0, z_rows)
    fill(z_slopes, vz)
    transform(1, z_slopes)
    distance = lax.broadcasted_iota(jnp.int32, (16, atoms), 0) - (cell_ref[0:1, :] - r * CX)
    x_rows[0] = pick(distance, wx)
    x_rows[1] = pick(distance, vx)
    distance = lax.broadcasted_iota(jnp.int32, (HALO_ROWS, atoms), 0) - (
        cell_ref[1:2, :] - c * CY
    )
    y_rows[0] = pick(distance, wy)
    y_rows[1] = pick(distance, vy)
    plane[:, TOP:, :] = jnp.zeros((2, PLANE - TOP, atoms), jnp.bfloat16)

    for copy in frags:
        copy.wait()
    total = frag_in[0]
    for k in range(1, len(diffs)):
        total = total + frag_in[k]
    mean = jnp.where(tile_lane[:1] < count * S_DEV, total[0:1] / total[1:2], 0.0)
    mean = jnp.concatenate(thirds(mean) + [jnp.zeros((13, LANES), jnp.float32)], axis=0)
    mean = one_dot(mean.astype(jnp.bfloat16), member[...])
    mean = mean[0:1] + mean[1:2] + mean[2:3]
    neutral = (charges - mean) * live

    x_charged = x_rows[0, :CX] * neutral
    for y in range(0, EXT_Y - 1, 2):
        pair = jnp.concatenate(
            [y_rows[0, y : y + 1, :] * x_charged, y_rows[0, y + 1 : y + 2, :] * x_charged], axis=0
        )
        plane[0, y * CX : (y + 2) * CX, :], plane[1, y * CX : (y + 2) * CX, :] = split(pair)
    base = EXT_Y * CX
    y_charged = y_rows[0] * neutral
    tail = [y_rows[0, EXT_Y - 1 : EXT_Y, :] * x_charged]
    for x in range(3):
        tail.append(x_rows[0, CX + x : CX + x + 1, :] * y_charged)
    tail = jnp.concatenate(tail, axis=0)
    plane[0, base - CX : TOP, :], plane[1, base - CX : TOP, :] = split(tail)

    per = lines // n

    def spread_out(values, target):
        for p in range(n):
            target[p] = values[per * p : per * (p + 1)]

    def gathered(source):
        return jnp.concatenate([source[p] for p in range(n)], axis=0)

    def send(source, target, index):
        for o in far_first:
            pltpu.make_async_remote_copy(
                source.at[other(o)], target.at[me], send_sems.at[index], recv_sems.at[index],
                device_id=peer(o), device_id_type=MESH,
            ).start()
        target[me] = source[me]

    def whole(source, target, send_sem, recv_sem):
        return pltpu.make_async_remote_copy(
            source.at[pl.ds(0, n - 1)], target.at[pl.ds(0, n - 1)], send_sem, recv_sem,
            device_id=(r, c), device_id_type=MESH,
        )

    part_lane = lax.broadcasted_iota(jnp.int32, (lines, LANES), 1)
    third = PLANE - TOP

    def lent(values, extra, k):
        tail = values[:, LANES:]
        moved = pltpu.roll(extra, LANES - third * (k + 1), 1)
        return jnp.concatenate(
            [values[:, :LANES], jnp.where(part_lane < LANES - third, tail, moved)], axis=1
        )

    def returned(tails):
        result = pltpu.roll(tails[-1], third * CHUNKS - third, 1)
        for k in range(CHUNKS - 2, -1, -1):
            result = jnp.where(
                part_lane < third * (k + 1), pltpu.roll(tails[k], third * (k + 1), 1), result
            )
        return result

    last = CHUNKS - 1

    def field_of(chunks):
        rows_of = [
            jnp.concatenate(
                [zf[0, half, ch * lines : (ch + 1) * lines, :] for ch in chunks], axis=0
            )
            for half in range(2)
        ]
        value = tall_dot(rows_of, (plane[0], plane[1]), (1, 1))
        return [value[i * lines : (i + 1) * lines] for i in range(len(chunks))]

    first, end = field_of([0, last])
    end_tail = end[:, LANES:]
    spread_out(lent(first, end_tail, 0), field_out.at[0])
    send(field_out.at[0], field_in.at[0], 0)
    middle = field_of(list(range(1, last)))
    for ch in range(1, last):
        spread_out(lent(middle[ch - 1], end_tail, ch), field_out.at[ch])
        send(field_out.at[ch], field_in.at[ch], ch)
    spread_out(end[:, :LANES], field_end)
    send(field_end, field_end_in, last)

    whole(inf_out, inf_in, inf_send, inf_recv).wait()
    copies[12].wait()
    group = lax.broadcasted_iota(jnp.int32, (8, LANES), 1) % rows
    wanted = group == lax.broadcasted_iota(jnp.int32, (8, LANES), 0)
    for t in range(8):
        blocks = []
        for m in range(cols):
            row = (t % 2) * cols + m
            blocks.append(jnp.concatenate(
                [
                    jnp.where(wanted, inf_in[t // 2 * rows + q, row : row + 1, :], 0.0)
                    for q in range(rows)
                ],
                axis=1,
            ))
        high, low = split(jnp.concatenate(blocks, axis=0))
        green[t] = one_dot(high, spot[...]) + one_dot(low, spot[...])

    for copy in copies[7:12]:
        copy.wait()

    for ch in range(CHUNKS):
        if ch < last:
            whole(field_out.at[ch], field_in.at[ch], send_sems.at[ch], recv_sems.at[ch]).wait()
            arrived = gathered(field_in.at[ch])
        else:
            whole(field_end, field_end_in, send_sems.at[ch], recv_sems.at[ch]).wait()
            tails = [gathered(field_in.at[k])[:, LANES:] for k in range(last)]
            arrived = jnp.concatenate([gathered(field_end_in), returned(tails)], axis=1)
        mixed = one_dot(wide[ch], tripled_rows(arrived))
        repeats = lines // n
        cosine = jnp.concatenate([twiddle[0]] * repeats, axis=0)
        sine = jnp.concatenate([twiddle[1]] * repeats, axis=0)
        real, imag = mixed[:lines], mixed[lines:]
        turned = jnp.concatenate(
            [real * cosine + imag * sine, imag * cosine - real * sine], axis=1
        )
        spectrum = tall_dot(split(turned), (inner_t[0], inner_t[1]))
        slots = [
            jnp.where(me == 0, t0, t1) for t0, t1 in zip(slot_lists(0)[ch], slot_lists(1)[ch])
        ]
        kernel_values = jnp.concatenate([green[t] for t in slots], axis=0)
        filtered = spectrum * jnp.concatenate([kernel_values, kernel_values], axis=1)
        back = tall_dot(split(filtered), (inner[0], inner[1]))
        real, imag = back[:, :PLANE], back[:, PLANE:]
        turned = jnp.concatenate(
            [real * cosine - imag * sine, imag * cosine + real * sine], axis=0
        )
        value = one_dot(gather[ch], tripled_rows(turned))
        if ch == 0:
            spare[...] = value[:, LANES:]
            spread_out(value[:, :LANES], back_end)
            send(back_end, back_end_in, CHUNKS)
        else:
            spread_out(lent(value, spare[...], ch - 1), back_out.at[ch - 1])
            send(back_out.at[ch - 1], back_in.at[ch - 1], CHUNKS + ch)

    scale = 1.0 / float(CX * rows * CY * cols * NZ)

    def down(values):
        return jnp.sum(values, axis=0, keepdims=True)

    def turned_rows(values):
        found = (values * scale).T
        high = found.astype(jnp.bfloat16).astype(jnp.float32)
        return jnp.concatenate([high, found - high, high], axis=1).astype(jnp.bfloat16)

    inside, outside = {}, {}
    sums = [[0.0] * 4 for _ in range(atoms // width)]
    for ch in range(1, CHUNKS):
        if ch == 1:
            whole(back_end, back_end_in, send_sems.at[CHUNKS], recv_sems.at[CHUNKS]).wait()
            inside[0] = turned_rows(gathered(back_end_in))
        index = CHUNKS + ch
        whole(
            back_out.at[ch - 1], back_in.at[ch - 1], send_sems.at[index], recv_sems.at[index]
        ).wait()
        arrived = gathered(back_in.at[ch - 1])
        both = turned_rows(arrived)
        inside[ch], outside[ch] = both[:LANES], both[LANES:TOP]
        if ch == last:
            tails = [gathered(back_in.at[k])[:, LANES:] for k in range(last)]
            outside[0] = turned_rows(returned(tails))[: TOP - LANES]
        for k in range(atoms // width):
            cut = slice(k * width, (k + 1) * width)
            for which in range(2):
                def stacked(c):
                    near = zf[which, 0, c * lines : (c + 1) * lines, cut]
                    far = zf[which, 1, c * lines : (c + 1) * lines, cut]
                    return jnp.concatenate([near, near, far], axis=0)

                here = one_dot(inside[ch], stacked(ch))
                if ch == 1:
                    here = here + one_dot(inside[0], stacked(0))
                there = one_dot(outside[ch], stacked(ch))
                if ch == last:
                    there = there + one_dot(outside[0], stacked(0))
                sampled[which, :LANES, cut] = here
                sampled[which, LANES:, cut] = there
            by_y = by_dy = by_yz = 0.0
            for y in range(EXT_Y):
                row = slice(y * CX, (y + 1) * CX)
                weight = y_rows[0, y : y + 1, cut]
                by_y = by_y + weight * sampled[0, row, cut]
                by_dy = by_dy + y_rows[1, y : y + 1, cut] * sampled[0, row, cut]
                by_yz = by_yz + weight * sampled[1, row, cut]
            by_x = by_dx = by_xz = 0.0
            for x in range(3):
                row = slice(base + x * HALO_ROWS, base + (x + 1) * HALO_ROWS)
                weight = x_rows[0, CX + x : CX + x + 1, cut]
                by_x = by_x + weight * sampled[0, row, cut]
                by_dx = by_dx + x_rows[1, CX + x : CX + x + 1, cut] * sampled[0, row, cut]
                by_xz = by_xz + weight * sampled[1, row, cut]
            xs, dxs = x_rows[0, :CX, cut], x_rows[1, :CX, cut]
            ys, dys = y_rows[0, :, cut], y_rows[1, :, cut]
            found = [
                down(xs * by_y) + down(ys * by_x),
                down(dxs * by_y) + down(ys * by_dx),
                down(xs * by_dy) + down(dys * by_x),
                down(xs * by_yz) + down(ys * by_xz),
            ]
            sums[k] = [a + b for a, b in zip(sums[k], found)]
    for k in range(atoms // width):
        cut = slice(k * width, (k + 1) * width)
        part = neutral[:, cut]
        value, grad_x, grad_y, grad_z = sums[k]
        energy_ref[:, cut] = 0.5 * part * value
        forces_ref[0:1, cut] = -part * grad_x
        forces_ref[1:2, cut] = -part * grad_y
        forces_ref[2:3, cut] = -part * grad_z


def put(forces_ref, energy_ref, forces_out, energy_out, sems):
    copies = [
        pltpu.make_async_copy(forces_ref, forces_out, sems.at[0]),
        pltpu.make_async_copy(energy_ref, energy_out, sems.at[1]),
    ]
    for copy in copies:
        copy.start()
    for copy in copies:
        copy.wait()


def fast_body(plan, charges, structure_id, live_count, cell_index, fraction, influence):
    rows, cols, offsets, diffs = plan
    n = rows * cols
    atoms = charges.shape[0]
    tables = make_tables(rows, cols)
    vmem = pl.BlockSpec(memory_space=pltpu.VMEM)
    anywhere = pl.BlockSpec(memory_space=pltpu.HBM)
    f32, bf16 = jnp.float32, jnp.bfloat16
    stored = influence.reshape(2, n, CX, CX * rows)
    inputs = [
        charges[None, :], structure_id[None, :], live_count, cell_index, fraction, stored,
    ]
    held = [
        pltpu.SMEM(v.shape, v.dtype) if v is live_count else pltpu.VMEM(v.shape, v.dtype)
        for v in inputs
    ]
    for i, table in enumerate(tables):
        held.append(pltpu.VMEM(table.shape[1:] if i in (1, 2) else table.shape, table.dtype))
    sems = pltpu.SemaphoreType.DMA
    exchanged = pltpu.VMEM((CHUNKS - 1, n, NZ // CHUNKS // n, PLANE), f32)
    short = pltpu.VMEM((n, NZ // CHUNKS // n, LANES), f32)
    forces, energy = pl.pallas_call(
        functools.partial(kernel, plan),
        out_shape=(
            pltpu.VMEM((3, atoms), f32),
            pltpu.VMEM((1, atoms), f32),
        ),
        in_specs=[anywhere] * (len(inputs) + len(tables)),
        out_specs=(vmem, vmem),
        scratch_shapes=held + [
            pltpu.VMEM((2, NZ, atoms), bf16),
            pltpu.VMEM((2, NZ, atoms), bf16),
            pltpu.VMEM((2, 2, NZ, atoms), bf16),
            pltpu.VMEM((2, PLANE, atoms), bf16),
            pltpu.VMEM((2, 16, atoms), f32),
            pltpu.VMEM((2, HALO_ROWS, atoms), f32),
            pltpu.VMEM((LANES, atoms), bf16),
            pltpu.VMEM((len(diffs), 2, LANES), f32),
            pltpu.VMEM((len(diffs), 2, LANES), f32),
            pltpu.VMEM((n, 8, LANES), f32),
            pltpu.VMEM((n, 8, LANES), f32),
            pltpu.VMEM((8, n, LANES), f32),
            exchanged, exchanged, short, short, exchanged, exchanged, short, short,
            pltpu.VMEM((NZ // CHUNKS, LANES), f32),
            pltpu.VMEM((2, TOP, atoms), f32),
            sems((len(held),)),
            sems((len(diffs),)), sems((len(diffs),)), sems(()), sems(()),
            sems((2 * CHUNKS,)), sems((2 * CHUNKS,)),
        ],
        compiler_params=pltpu.CompilerParams(
            collective_id=0, has_side_effects=True, vmem_limit_bytes=66000000
        ),
        name="ewald_step",
    )(*inputs, *[jnp.asarray(t) for t in tables])
    forces, energy = pl.pallas_call(
        put,
        out_shape=(
            jax.ShapeDtypeStruct((3, atoms), f32),
            jax.ShapeDtypeStruct((1, atoms), f32),
        ),
        in_specs=[vmem] * 2,
        out_specs=(anywhere, anywhere),
        scratch_shapes=[sems((2,))],
        compiler_params=pltpu.CompilerParams(vmem_limit_bytes=262144),
        name="put_results",
    )(forces, energy)
    return forces, energy[0]


def solution(mesh):
    plan = make_plan(mesh.shape["row"], mesh.shape["col"])
    placed = (
        P(("row", "col")),
        P(("row", "col")),
        P(("row", "col")),
        P(None, ("row", "col")),
        P(None, ("row", "col")),
        P("col", "row", None),
    )
    return jax.shard_map(
        body if plan is None else functools.partial(fast_body, plan),
        mesh=mesh,
        in_specs=placed,
        out_specs=(P(None, ("row", "col")), P(("row", "col"))),
        check_vma=False,
    )
```

```python
import math

import functools

import jax
import jax.numpy as jnp
import numpy as np
from jax import lax
from jax.experimental import pallas as pl
from jax.experimental.pallas import tpu as pltpu
from jax.sharding import PartitionSpec as P

CX = 8
CY = 16
NZ = 256
S_DEV = 8


highest = lax.Precision.HIGHEST


def passed_along(block, axis, distance):
    devices = range(lax.axis_size(axis))
    route = [((i - distance) % len(devices), i) for i in devices]
    return lax.ppermute(block, axis, route)


def spline_weights(fraction):
    remain = 1.0 - fraction
    square = fraction * fraction
    cubic_term = square * fraction
    values = [
        remain * remain * remain / 6.0,
        (3.0 * cubic_term - 6.0 * square + 4.0) / 6.0,
        (-3.0 * cubic_term + 3.0 * square + 3.0 * fraction + 1.0) / 6.0,
        cubic_term / 6.0,
    ]
    slopes = [
        -0.5 * remain * remain,
        0.5 * (3.0 * square - 4.0 * fraction),
        0.5 * (-3.0 * square + 2.0 * fraction + 1.0),
        0.5 * square,
    ]
    return (values, slopes)


def place_weights(weights, local, width, period):
    columns = lax.broadcasted_iota(jnp.int32, (local.shape[0], width), 1)
    result = jnp.zeros((local.shape[0], width), jnp.float32)
    for offset in range(4):
        target = (local + offset) % period
        result = result + jnp.where(columns == target[:, None], weights[offset][:, None], 0.0)
    return result


def dft_tables(length):
    counter = lax.iota(jnp.int32, length)
    product = counter[:, None] * counter[None, :] % length
    angle = 2.0 * math.pi / length * product.astype(jnp.float32)
    return (jnp.cos(angle), jnp.sin(angle))


def rotate_pair(real_part, imag_part, pattern, cosine, sine, direction):
    real_cos = jnp.einsum(pattern, real_part, cosine, precision=highest)
    real_sin = jnp.einsum(pattern, real_part, sine, precision=highest)
    imag_cos = jnp.einsum(pattern, imag_part, cosine, precision=highest)
    imag_sin = jnp.einsum(pattern, imag_part, sine, precision=highest)
    return (real_cos - direction * imag_sin, imag_cos + direction * real_sin)


def body(charges, structure_id, live_count, cell_index, fraction, influence):
    atom_total = charges.shape[0]
    row_count = lax.axis_size("row")
    col_count = lax.axis_size("col")
    mesh_x = CX * row_count
    mesh_y = CY * col_count
    structures = S_DEV * row_count * col_count
    local_x = cell_index[0] - lax.axis_index("row") * CX
    local_y = cell_index[1] - lax.axis_index("col") * CY
    live = (lax.iota(jnp.int32, atom_total) < live_count[0]).astype(jnp.float32)
    wx_val, wx_slope = spline_weights(fraction[0])
    wy_val, wy_slope = spline_weights(fraction[1])
    wz_val, wz_slope = spline_weights(fraction[2])
    big_period = 4 * (CX + CY + 8)
    x_rows = place_weights(wx_val, local_x, CX + 3, big_period)
    x_slope_rows = place_weights(wx_slope, local_x, CX + 3, big_period)
    y_rows = place_weights(wy_val, local_y, CY + 3, big_period)
    y_slope_rows = place_weights(wy_slope, local_y, CY + 3, big_period)
    z_rows = place_weights(wz_val, cell_index[2], NZ, NZ)
    z_slope_rows = place_weights(wz_slope, cell_index[2], NZ, NZ)
    plane = (y_rows[:, :, None] * x_rows[:, None, :]).reshape(atom_total, -1)
    charge_sums = jax.ops.segment_sum(charges * live, structure_id, num_segments=structures)
    live_sums = jax.ops.segment_sum(live, structure_id, num_segments=structures)
    totals, counts = lax.psum((charge_sums, live_sums), ("row", "col"))
    neutral = (charges - jnp.take(totals / counts, structure_id)) * live
    spread_grid = lax.dot_general(
        plane,
        neutral[:, None] * z_rows,
        (((0,), (0,)), ((), ())),
        precision=highest,
        preferred_element_type=jnp.float32,
    )
    extended = spread_grid.reshape(CY + 3, CX + 3, NZ)
    spill_x = passed_along(extended[:, CX:, :], "row", 1)
    extended = extended[:, :CX, :].at[:, :3, :].add(spill_x)
    spill_y = passed_along(extended[CY:], "col", 1)
    density = extended[:CY].at[:3].add(spill_y)
    cos_z, sin_z = dft_tables(NZ)
    cos_y, sin_y = dft_tables(mesh_y)
    cos_x, sin_x = dft_tables(mesh_x)
    real_z = jnp.einsum("yxz,zk->kxy", density, cos_z, precision=highest)
    imag_z = -jnp.einsum("yxz,zk->kxy", density, sin_z, precision=highest)
    columns = lax.all_to_all(
        jnp.stack([real_z, imag_z]), "col", split_axis=1, concat_axis=3, tiled=True
    )
    real_y, imag_y = rotate_pair(columns[0], columns[1], "zxy,yk->zkx", cos_y, sin_y, -1.0)
    rows = lax.all_to_all(
        jnp.stack([real_y, imag_y]), "row", split_axis=2, concat_axis=3, tiled=True
    )
    real_x, imag_x = rotate_pair(rows[0], rows[1], "zyx,xk->zyk", cos_x, sin_x, -1.0)
    scale = influence / float(mesh_x * mesh_y * NZ)
    real_x = real_x * scale
    imag_x = imag_x * scale
    back_x, back_x_imag = rotate_pair(real_x, imag_x, "zyk,kx->zyx", cos_x, sin_x, 1.0)
    returned = lax.all_to_all(
        jnp.stack([back_x, back_x_imag]), "row", split_axis=3, concat_axis=2, tiled=True
    )
    back_y, back_y_imag = rotate_pair(returned[0], returned[1], "zkx,ky->zxy", cos_y, sin_y, 1.0)
    whole_z = lax.all_to_all(
        jnp.stack([back_y, back_y_imag]), "col", split_axis=3, concat_axis=1, tiled=True
    )
    potential = jnp.einsum("kxy,kz->yxz", whole_z[0], cos_z, precision=highest) - jnp.einsum(
        "kxy,kz->yxz", whole_z[1], sin_z, precision=highest
    )
    upper_x = passed_along(potential[:, :3, :], "row", -1)
    widened = jnp.concatenate([potential, upper_x], axis=1)
    upper_y = passed_along(widened[:3], "col", -1)
    widened = jnp.concatenate([widened, upper_y], axis=0).reshape(-1, NZ)
    sampled = lax.dot_general(
        jnp.concatenate([z_rows, z_slope_rows], axis=0),
        widened,
        (((1,), (1,)), ((), ())),
        precision=highest,
        preferred_element_type=jnp.float32,
    )
    sample_val = sampled[:atom_total]
    sample_slope = sampled[atom_total:]
    plane_dx = (y_rows[:, :, None] * x_slope_rows[:, None, :]).reshape(atom_total, -1)
    plane_dy = (y_slope_rows[:, :, None] * x_rows[:, None, :]).reshape(atom_total, -1)
    value = jnp.sum(plane * sample_val, axis=1)
    grad_x = jnp.sum(plane_dx * sample_val, axis=1)
    grad_y = jnp.sum(plane_dy * sample_val, axis=1)
    grad_z = jnp.sum(plane * sample_slope, axis=1)
    atom_energy = 0.5 * neutral * value
    forces = -neutral[None, :] * jnp.stack([grad_x, grad_y, grad_z])
    return (forces, atom_energy)


EXT_Y = CY + 3
HALO_ROWS = 24
PLANE = 256
LANES = 128
TOP = EXT_Y * CX + 3 * HALO_ROWS
CHUNKS = 4
MESH = pl.DeviceIdType.MESH


def plane_cells():
    cells = np.zeros((PLANE, 2), np.int64)
    used = np.zeros((PLANE,), bool)
    for y in range(EXT_Y):
        for x in range(CX):
            cells[y * CX + x] = (x, y)
            used[y * CX + x] = True
    for x in range(3):
        for y in range(EXT_Y):
            cells[EXT_Y * CX + x * HALO_ROWS + y] = (CX + x, y)
            used[EXT_Y * CX + x * HALO_ROWS + y] = True
    return cells, used


def make_plan(rows, cols):
    n = rows * cols
    offsets = [(0, 0), (1, 0), (-1, 0), (0, 1), (0, -1), (rows // 2, 0)]
    distinct = len({(a % rows, b % cols) for a, b in offsets}) == len(offsets)
    if not (
        rows % 2 == 0
        and cols % 2 == 0
        and rows & (rows - 1) == 0
        and cols & (cols - 1) == 0
        and distinct
        and (CY * cols) % rows == 0
        and CY == 2 * rows
        and CX == 8
        and NZ == 8 * n
        and NZ // cols == 2 * n
        and 4 * n == LANES
        and cols == 4
    ):
        return None
    diffs = [(0, 0)]
    for a, b in offsets:
        for d, e in offsets:
            diff = ((a - d) % rows, (b - e) % cols)
            if diff not in diffs:
                diffs.append(diff)
    return (rows, cols, tuple(offsets), tuple(diffs))


def slot_lists(kind):
    if kind:
        return ((0, 7), (1, 6), (2, 5), (3, 4))
    return ((0, 4), (1, 7), (2, 6), (3, 5))


def make_tables(rows, cols):
    n = rows * cols
    half = NZ // n // 2
    slots = 2 * half
    z = np.arange(NZ)
    forward_z = np.zeros((n, 2, half, NZ))
    for p in range(n):
        for j in range(half):
            angle = 2 * np.pi * ((p + n * j) * z % NZ) / NZ
            forward_z[p, 0, j] = np.cos(angle)
            forward_z[p, 1, j] = -np.sin(angle)
    forward_z[0, 1, 0] = 1.0 - 2.0 * (z % 2)
    per_chunk = half // CHUNKS
    forward_z = forward_z.reshape(n, 2, CHUNKS, per_chunk, NZ).transpose(2, 0, 1, 3, 4)
    forward_z = forward_z.reshape(NZ, NZ)

    r, c, m1, k1 = np.meshgrid(
        np.arange(rows), np.arange(cols), np.arange(cols), np.arange(rows), indexing="ij"
    )
    phi = 2 * np.pi * ((k1 * r % rows) / rows + (m1 * c % cols) / cols)
    phi = phi.reshape(n, n)
    cosp, sinp = np.cos(phi), np.sin(phi)
    gather = np.zeros((2, n, 2, half, 2, slots, n))
    for kind in range(2):
        for t in range(slots):
            j, sign = t, 1.0
            if t >= half:
                j, sign = (slots - 1 - t if kind else slots - t), -1.0
            if kind == 0 and t in (0, half):
                part = 0 if t == 0 else 1
                gather[kind, :, part, 0, 0, t] = cosp
                gather[kind, :, part, 0, 1, t] = -sinp
                continue
            gather[kind, :, 0, j, 0, t] = cosp
            gather[kind, :, 1, j, 0, t] = sign * sinp
            gather[kind, :, 0, j, 1, t] = -sinp
            gather[kind, :, 1, j, 1, t] = sign * cosp
    chunked = np.zeros((2, CHUNKS, n, 2, per_chunk, 2, slots // CHUNKS, n))
    for kind in range(2):
        for ch in range(CHUNKS):
            js = slice(ch * per_chunk, (ch + 1) * per_chunk)
            chunked[kind, ch] = gather[kind][:, :, js][:, :, :, :, list(slot_lists(kind)[ch])]
    lines = 2 * per_chunk * n
    gather = chunked.reshape(2, CHUNKS, lines, 2 * slots // CHUNKS * n)

    cells, used = plane_cells()
    x, y = cells[:, 0], cells[:, 1]
    low_m, low_k = (v.reshape(-1) for v in np.meshgrid(np.arange(cols), np.arange(rows), indexing="ij"))
    psi = 2 * np.pi * (
        x[None] * low_k[:, None] / (CX * rows) + y[None] * low_m[:, None] / (CY * cols)
    )
    twiddle = np.stack([np.cos(psi), np.sin(psi)])
    high_m, high_k = (v.reshape(-1) for v in np.meshgrid(np.arange(CY), np.arange(CX), indexing="ij"))
    chi = 2 * np.pi * (high_k[:, None] * x[None] % CX / CX + high_m[:, None] * y[None] % CY / CY)
    cosc, sinc = np.cos(chi) * used[None], np.sin(chi) * used[None]
    inner = np.block([[cosc, sinc], [-sinc, cosc]])
    width = CX * rows
    source = np.arange(rows * 2 * width)
    spot = (source // width) * CX + source % width // rows
    place = (spot[:, None] == np.arange(CY * CX)[None]).astype(np.float32)

    def pair(table, axis):
        table = np.asarray(table, np.float32)
        high = table.astype(jnp.bfloat16)
        low = (table - high.astype(np.float32)).astype(jnp.bfloat16)
        return np.stack([high, low], axis=axis)

    def tripled(table):
        high, low = pair(table, 0)
        return np.concatenate([high, low, high], axis=-1)

    return (
        pair(forward_z, 0),
        tripled(gather.transpose(0, 1, 3, 2)),
        tripled(gather),
        twiddle.astype(np.float32),
        pair(inner.T, 0),
        pair(inner, 0),
        place.astype(jnp.bfloat16),
    )


def split(values):
    high = values.astype(jnp.bfloat16)
    return high, (values - high.astype(jnp.float32)).astype(jnp.bfloat16)


def one_dot(a, b, contract=(1, 0)):
    return lax.dot_general(
        a, b, ((contract[:1], contract[1:]), ((), ())), preferred_element_type=jnp.float32
    )


def dot(left, right, contract=(1, 0)):
    return one_dot(left[0], right[0], contract) + (
        one_dot(left[0], right[1], contract) + one_dot(left[1], right[0], contract)
    )


def tall_dot(left, right, contract=(1, 0)):
    height = left[0].shape[0]
    stacked = one_dot(jnp.concatenate(left, axis=0), right[0], contract)
    return stacked[:height] + (stacked[height:] + one_dot(left[0], right[1], contract))


def tripled_rows(values):
    high, low = split(values)
    return jnp.concatenate([high, high, low], axis=0)


def pick(distance, weights):
    result = jnp.where(distance == 3, weights[3], 0.0)
    for i in (2, 1, 0):
        result = jnp.where(distance == i, weights[i], result)
    return result


def kernel(
    plan,
    charges_hbm, sid_hbm, live_hbm, cell_hbm, frac_hbm, influence_hbm,
    fz_hbm, wide_hbm, gather_hbm, twiddle_hbm, inner_t_hbm, inner_hbm, place_hbm,
    forces_ref, energy_ref,
    charges_ref, sid_ref, live_ref, cell_ref, frac_ref, raw,
    fz, wide, gather, twiddle, inner_t, inner, spot,
    z_rows, z_slopes, zf, plane, x_rows, y_rows,
    member, frag_out, frag_in, inf_out, inf_in, green,
    field_out, field_in, field_end, field_end_in, back_out, back_in, back_end, back_end_in,
    spare, sampled,
    local_sems, frag_send, frag_recv, inf_send, inf_recv, send_sems, recv_sems,
):
    rows, cols, offsets, diffs = plan
    n = rows * cols
    r, c = lax.axis_index("row"), lax.axis_index("col")
    me = r * cols + c
    atoms = charges_ref.shape[1]
    lines = NZ // CHUNKS
    kind = jnp.minimum(me, 1)
    far_first = sorted(range(1, n), key=lambda o: o)

    def other(o):
        return lax.rem(me + o, n)

    def peer(o):
        return (lax.div(other(o), cols), lax.rem(other(o), cols))

    barrier = pltpu.get_barrier_semaphore()
    for o in far_first:
        pl.semaphore_signal(barrier, inc=1, device_id=peer(o), device_id_type=MESH)

    copies = [
        pltpu.make_async_copy(source, target, local_sems.at[i])
        for i, (source, target) in enumerate([
            (charges_hbm, charges_ref),
            (sid_hbm, sid_ref),
            (live_hbm, live_ref),
            (frac_hbm, frac_ref),
            (cell_hbm, cell_ref),
            (influence_hbm, raw),
            (fz_hbm, fz),
            (wide_hbm.at[kind], wide),
            (gather_hbm.at[kind], gather),
            (twiddle_hbm, twiddle),
            (inner_t_hbm, inner_t),
            (inner_hbm, inner),
            (place_hbm, spot),
        ])
    ]
    for copy in copies:
        copy.start()

    for copy in copies[:3]:
        copy.wait()
    lane = lax.broadcasted_iota(jnp.int32, (1, atoms), 1)
    live = (lane < live_ref[0]).astype(jnp.float32)
    charges = charges_ref[...]
    charged = charges * live
    sid = sid_ref[...]
    within = lax.broadcasted_iota(jnp.int32, (S_DEV, atoms), 0)
    count = len(offsets)
    held = [
        sid == within + S_DEV * (
            lax.rem(r + a % rows, rows) * cols + lax.rem(c + b % cols, cols)
        )
        for a, b in offsets
    ]
    for i in range(0, count, 2):
        chosen = jnp.concatenate([jnp.where(h, 1.0, 0.0) for h in held[i : i + 2]], axis=0)
        member[i * S_DEV : (i + 2) * S_DEV, :] = chosen.astype(jnp.bfloat16)
    member[count * S_DEV :, :] = jnp.zeros((LANES - count * S_DEV, atoms), jnp.bfloat16)

    def thirds(values):
        first = values.astype(jnp.bfloat16).astype(jnp.float32)
        second = (values - first).astype(jnp.bfloat16).astype(jnp.float32)
        return [first, second, values - first - second]

    weighed = thirds(charged) + [live, jnp.zeros((12, atoms), jnp.float32)]
    weighed = jnp.concatenate(weighed, axis=0).astype(jnp.bfloat16)
    local_sums = one_dot(weighed, member[...], (1, 1))
    local_sums = jnp.concatenate(
        [
            local_sums[0:1] + local_sums[1:2] + local_sums[2:3],
            local_sums[3:4],
            jnp.zeros((6, LANES), jnp.float32),
        ],
        axis=0,
    )
    tile_lane = lax.broadcasted_iota(jnp.int32, (8, LANES), 1)
    shifted = {
        k: local_sums if k == 0 else pltpu.roll(local_sums, S_DEV * k % LANES, 1)
        for k in range(1 - count, count)
    }
    messages = [jnp.zeros((8, LANES), jnp.float32) for _ in diffs]
    for j, (a, b) in enumerate(offsets):
        for i, (d, e) in enumerate(offsets):
            k = diffs.index(((a - d) % rows, (b - e) % cols))
            messages[k] = jnp.where(tile_lane // S_DEV == j, shifted[j - i], messages[k])
    frag_in[0] = messages[0][:2]
    for k in range(1, len(diffs)):
        frag_out[k] = messages[k][:2]

    for copy in copies[3:5]:
        copy.wait()
    wx, vx = spline_weights(frac_ref[0:1, :])
    wy, vy = spline_weights(frac_ref[1:2, :])
    wz, vz = spline_weights(frac_ref[2:3, :])
    cell_z = cell_ref[2:3, :]
    step = 16

    def fill(target, weights):
        @pl.loop(0, NZ // step)
        def _(b):
            start = pl.multiple_of(b * step, step)
            index = lax.broadcasted_iota(jnp.int32, (step, atoms), 0) + start - cell_z
            distance = jnp.where(index < 0, index + NZ, index)
            target[0, pl.ds(start, step), :], target[1, pl.ds(start, step), :] = split(
                pick(distance, weights)
            )

    width = 256

    def transform(which, source):
        for k in range(atoms // width):
            cut = slice(k * width, (k + 1) * width)
            value = dot((fz[0], fz[1]), (source[0, :, cut], source[1, :, cut]))
            zf[which, 0, :, cut], zf[which, 1, :, cut] = split(value)

    fill(z_rows, wz)
    copies[5].wait()
    for p in range(n):
        first, second = raw[0, p], raw[1, p]
        low = jnp.concatenate([first[:4], second[:4]], axis=0)
        high = jnp.concatenate([first[4:], second[4:]], axis=0)
        inf_out[p] = jnp.concatenate([low, high], axis=1)

    pl.semaphore_wait(barrier, n - 1)

    def frag_copy(k):
        a, b = diffs[k]
        target = (lax.rem(r + (-a) % rows, rows), lax.rem(c + (-b) % cols, cols))
        return pltpu.make_async_remote_copy(
            frag_out.at[k], frag_in.at[k], frag_send.at[k], frag_recv.at[k],
            device_id=target, device_id_type=MESH,
        )

    frags = [frag_copy(k) for k in range(1, len(diffs))]
    for copy in frags:
        copy.start()

    place = c * rows + r

    def residue(p):
        return jnp.where(c < cols // 2, p, lax.rem(n - p, n))

    for o in far_first:
        pltpu.make_async_remote_copy(
            inf_out.at[residue(other(o))], inf_in.at[place], inf_send, inf_recv,
            device_id=peer(o), device_id_type=MESH,
        ).start()
    inf_in[place] = inf_out[residue(me)]

    copies[6].wait()
    transform(0, z_rows)
    distance = lax.broadcasted_iota(jnp.int32, (16, atoms), 0) - (cell_ref[0:1, :] - r * CX)
    x_rows[0] = pick(distance, wx)
    x_rows[1] = pick(distance, vx)
    distance = lax.broadcasted_iota(jnp.int32, (HALO_ROWS, atoms), 0) - (
        cell_ref[1:2, :] - c * CY
    )
    y_rows[0] = pick(distance, wy)
    y_rows[1] = pick(distance, vy)
    plane[:, TOP:, :] = jnp.zeros((2, PLANE - TOP, atoms), jnp.bfloat16)

    for copy in frags:
        copy.wait()
    total = frag_in[0]
    for k in range(1, len(diffs)):
        total = total + frag_in[k]
    mean = jnp.where(tile_lane[:1] < count * S_DEV, total[0:1] / total[1:2], 0.0)
    mean = jnp.concatenate(thirds(mean) + [jnp.zeros((13, LANES), jnp.float32)], axis=0)
    mean = one_dot(mean.astype(jnp.bfloat16), member[...])
    mean = mean[0:1] + mean[1:2] + mean[2:3]
    neutral = (charges - mean) * live

    x_charged = x_rows[0, :CX] * neutral
    for y in range(0, EXT_Y - 1, 2):
        pair = jnp.concatenate(
            [y_rows[0, y : y + 1, :] * x_charged, y_rows[0, y + 1 : y + 2, :] * x_charged], axis=0
        )
        plane[0, y * CX : (y + 2) * CX, :], plane[1, y * CX : (y + 2) * CX, :] = split(pair)
    base = EXT_Y * CX
    y_charged = y_rows[0] * neutral
    tail = [y_rows[0, EXT_Y - 1 : EXT_Y, :] * x_charged]
    for x in range(3):
        tail.append(x_rows[0, CX + x : CX + x + 1, :] * y_charged)
    tail = jnp.concatenate(tail, axis=0)
    plane[0, base - CX : TOP, :], plane[1, base - CX : TOP, :] = split(tail)

    per = lines // n

    def spread_out(values, target):
        for p in range(n):
            target[p] = values[per * p : per * (p + 1)]

    def gathered(source):
        return jnp.concatenate([source[p] for p in range(n)], axis=0)

    def send(source, target, index):
        for o in far_first:
            pltpu.make_async_remote_copy(
                source.at[other(o)], target.at[me], send_sems.at[index], recv_sems.at[index],
                device_id=peer(o), device_id_type=MESH,
            ).start()
        target[me] = source[me]

    def whole(source, target, send_sem, recv_sem):
        return pltpu.make_async_remote_copy(
            source.at[pl.ds(0, n - 1)], target.at[pl.ds(0, n - 1)], send_sem, recv_sem,
            device_id=(r, c), device_id_type=MESH,
        )

    part_lane = lax.broadcasted_iota(jnp.int32, (lines, LANES), 1)
    third = PLANE - TOP

    def lent(values, extra, k):
        tail = values[:, LANES:]
        moved = pltpu.roll(extra, LANES - third * (k + 1), 1)
        return jnp.concatenate(
            [values[:, :LANES], jnp.where(part_lane < LANES - third, tail, moved)], axis=1
        )

    def returned(tails):
        result = pltpu.roll(tails[-1], third * CHUNKS - third, 1)
        for k in range(CHUNKS - 2, -1, -1):
            result = jnp.where(
                part_lane < third * (k + 1), pltpu.roll(tails[k], third * (k + 1), 1), result
            )
        return result

    last = CHUNKS - 1

    def field_of(chunks):
        rows_of = [
            jnp.concatenate(
                [zf[0, half, ch * lines : (ch + 1) * lines, :] for ch in chunks], axis=0
            )
            for half in range(2)
        ]
        value = tall_dot(rows_of, (plane[0], plane[1]), (1, 1))
        return [value[i * lines : (i + 1) * lines] for i in range(len(chunks))]

    first, end = field_of([0, last])
    end_tail = end[:, LANES:]
    spread_out(lent(first, end_tail, 0), field_out.at[0])
    send(field_out.at[0], field_in.at[0], 0)
    middle = field_of(list(range(1, last)))
    for ch in range(1, last):
        spread_out(lent(middle[ch - 1], end_tail, ch), field_out.at[ch])
        send(field_out.at[ch], field_in.at[ch], ch)
    spread_out(end[:, :LANES], field_end)
    send(field_end, field_end_in, last)

    fill(z_slopes, vz)
    transform(1, z_slopes)
    whole(inf_out, inf_in, inf_send, inf_recv).wait()
    copies[12].wait()
    group = lax.broadcasted_iota(jnp.int32, (8, LANES), 1) % rows
    wanted = group == lax.broadcasted_iota(jnp.int32, (8, LANES), 0)
    for t in range(8):
        blocks = []
        for m in range(cols):
            row = (t % 2) * cols + m
            blocks.append(jnp.concatenate(
                [
                    jnp.where(wanted, inf_in[t // 2 * rows + q, row : row + 1, :], 0.0)
                    for q in range(rows)
                ],
                axis=1,
            ))
        high, low = split(jnp.concatenate(blocks, axis=0))
        green[t] = one_dot(high, spot[...]) + one_dot(low, spot[...])

    for copy in copies[7:12]:
        copy.wait()

    for ch in range(CHUNKS):
        if ch < last:
            whole(field_out.at[ch], field_in.at[ch], send_sems.at[ch], recv_sems.at[ch]).wait()
            arrived = gathered(field_in.at[ch])
        else:
            whole(field_end, field_end_in, send_sems.at[ch], recv_sems.at[ch]).wait()
            tails = [gathered(field_in.at[k])[:, LANES:] for k in range(last)]
            arrived = jnp.concatenate([gathered(field_end_in), returned(tails)], axis=1)
        mixed = one_dot(wide[ch], tripled_rows(arrived))
        repeats = lines // n
        cosine = jnp.concatenate([twiddle[0]] * repeats, axis=0)
        sine = jnp.concatenate([twiddle[1]] * repeats, axis=0)
        real, imag = mixed[:lines], mixed[lines:]
        turned = jnp.concatenate(
            [real * cosine + imag * sine, imag * cosine - real * sine], axis=1
        )
        spectrum = tall_dot(split(turned), (inner_t[0], inner_t[1]))
        slots = [
            jnp.where(me == 0, t0, t1) for t0, t1 in zip(slot_lists(0)[ch], slot_lists(1)[ch])
        ]
        kernel_values = jnp.concatenate([green[t] for t in slots], axis=0)
        filtered = spectrum * jnp.concatenate([kernel_values, kernel_values], axis=1)
        back = tall_dot(split(filtered), (inner[0], inner[1]))
        real, imag = back[:, :PLANE], back[:, PLANE:]
        turned = jnp.concatenate(
            [real * cosine - imag * sine, imag * cosine + real * sine], axis=0
        )
        value = one_dot(gather[ch], tripled_rows(turned))
        if ch == 0:
            spare[...] = value[:, LANES:]
            spread_out(value[:, :LANES], back_end)
            send(back_end, back_end_in, CHUNKS)
        else:
            spread_out(lent(value, spare[...], ch - 1), back_out.at[ch - 1])
            send(back_out.at[ch - 1], back_in.at[ch - 1], CHUNKS + ch)

    scale = 1.0 / float(CX * rows * CY * cols * NZ)

    def down(values):
        return jnp.sum(values, axis=0, keepdims=True)

    def turned_rows(values):
        found = (values * scale).T
        high = found.astype(jnp.bfloat16).astype(jnp.float32)
        return jnp.concatenate([high, found - high, high], axis=1).astype(jnp.bfloat16)

    sums = [[0.0] * 4 for _ in range(atoms // width)]
    for ch in range(1, CHUNKS):
        piece = None
        if ch == 1:
            whole(back_end, back_end_in, send_sems.at[CHUNKS], recv_sems.at[CHUNKS]).wait()
            piece = turned_rows(gathered(back_end_in))
            piece_rows = slice(0, LANES)
        index = CHUNKS + ch
        whole(
            back_out.at[ch - 1], back_in.at[ch - 1], send_sems.at[index], recv_sems.at[index]
        ).wait()
        full = turned_rows(gathered(back_in.at[ch - 1]))[:TOP]
        if ch == last:
            tails = [gathered(back_in.at[k])[:, LANES:] for k in range(last)]
            piece = turned_rows(returned(tails))[: TOP - LANES]
            piece_rows = slice(LANES, TOP)
        for k in range(atoms // width):
            cut = slice(k * width, (k + 1) * width)
            for which in range(2):
                def stacked(c):
                    near = zf[which, 0, c * lines : (c + 1) * lines, cut]
                    far = zf[which, 1, c * lines : (c + 1) * lines, cut]
                    return jnp.concatenate([near, near, far], axis=0)

                most = one_dot(full, stacked(ch))
                if piece is None:
                    sampled[which, :, cut] = most
                    continue
                more = one_dot(piece, stacked(0))
                for part in (slice(0, LANES), slice(LANES, TOP)):
                    value = most[part]
                    sampled[which, part, cut] = value + more if part == piece_rows else value
            by_y = by_dy = by_yz = 0.0
            for y in range(EXT_Y):
                row = slice(y * CX, (y + 1) * CX)
                weight = y_rows[0, y : y + 1, cut]
                by_y = by_y + weight * sampled[0, row, cut]
                by_dy = by_dy + y_rows[1, y : y + 1, cut] * sampled[0, row, cut]
                by_yz = by_yz + weight * sampled[1, row, cut]
            by_x = by_dx = by_xz = 0.0
            for x in range(3):
                row = slice(base + x * HALO_ROWS, base + (x + 1) * HALO_ROWS)
                weight = x_rows[0, CX + x : CX + x + 1, cut]
                by_x = by_x + weight * sampled[0, row, cut]
                by_dx = by_dx + x_rows[1, CX + x : CX + x + 1, cut] * sampled[0, row, cut]
                by_xz = by_xz + weight * sampled[1, row, cut]
            xs, dxs = x_rows[0, :CX, cut], x_rows[1, :CX, cut]
            ys, dys = y_rows[0, :, cut], y_rows[1, :, cut]
            found = [
                down(xs * by_y) + down(ys * by_x),
                down(dxs * by_y) + down(ys * by_dx),
                down(xs * by_dy) + down(dys * by_x),
                down(xs * by_yz) + down(ys * by_xz),
            ]
            sums[k] = [a + b for a, b in zip(sums[k], found)]
    for k in range(atoms // width):
        cut = slice(k * width, (k + 1) * width)
        part = neutral[:, cut]
        value, grad_x, grad_y, grad_z = sums[k]
        energy_ref[:, cut] = 0.5 * part * value
        forces_ref[0:1, cut] = -part * grad_x
        forces_ref[1:2, cut] = -part * grad_y
        forces_ref[2:3, cut] = -part * grad_z


def put(forces_ref, energy_ref, forces_out, energy_out, sems):
    copies = [
        pltpu.make_async_copy(forces_ref, forces_out, sems.at[0]),
        pltpu.make_async_copy(energy_ref, energy_out, sems.at[1]),
    ]
    for copy in copies:
        copy.start()
    for copy in copies:
        copy.wait()


def fast_body(plan, charges, structure_id, live_count, cell_index, fraction, influence):
    rows, cols, offsets, diffs = plan
    n = rows * cols
    atoms = charges.shape[0]
    tables = make_tables(rows, cols)
    vmem = pl.BlockSpec(memory_space=pltpu.VMEM)
    anywhere = pl.BlockSpec(memory_space=pltpu.HBM)
    f32, bf16 = jnp.float32, jnp.bfloat16
    stored = influence.reshape(2, n, CX, CX * rows)
    inputs = [
        charges[None, :], structure_id[None, :], live_count, cell_index, fraction, stored,
    ]
    held = [
        pltpu.SMEM(v.shape, v.dtype) if v is live_count else pltpu.VMEM(v.shape, v.dtype)
        for v in inputs
    ]
    for i, table in enumerate(tables):
        held.append(pltpu.VMEM(table.shape[1:] if i in (1, 2) else table.shape, table.dtype))
    sems = pltpu.SemaphoreType.DMA
    exchanged = pltpu.VMEM((CHUNKS - 1, n, NZ // CHUNKS // n, PLANE), f32)
    short = pltpu.VMEM((n, NZ // CHUNKS // n, LANES), f32)
    forces, energy = pl.pallas_call(
        functools.partial(kernel, plan),
        out_shape=(
            pltpu.VMEM((3, atoms), f32),
            pltpu.VMEM((1, atoms), f32),
        ),
        in_specs=[anywhere] * (len(inputs) + len(tables)),
        out_specs=(vmem, vmem),
        scratch_shapes=held + [
            pltpu.VMEM((2, NZ, atoms), bf16),
            pltpu.VMEM((2, NZ, atoms), bf16),
            pltpu.VMEM((2, 2, NZ, atoms), bf16),
            pltpu.VMEM((2, PLANE, atoms), bf16),
            pltpu.VMEM((2, 16, atoms), f32),
            pltpu.VMEM((2, HALO_ROWS, atoms), f32),
            pltpu.VMEM((LANES, atoms), bf16),
            pltpu.VMEM((len(diffs), 2, LANES), f32),
            pltpu.VMEM((len(diffs), 2, LANES), f32),
            pltpu.VMEM((n, 8, LANES), f32),
            pltpu.VMEM((n, 8, LANES), f32),
            pltpu.VMEM((8, n, LANES), f32),
            exchanged, exchanged, short, short, exchanged, exchanged, short, short,
            pltpu.VMEM((NZ // CHUNKS, LANES), f32),
            pltpu.VMEM((2, TOP, atoms), f32),
            sems((len(held),)),
            sems((len(diffs),)), sems((len(diffs),)), sems(()), sems(()),
            sems((2 * CHUNKS,)), sems((2 * CHUNKS,)),
        ],
        compiler_params=pltpu.CompilerParams(
            collective_id=0, has_side_effects=True, vmem_limit_bytes=66000000
        ),
        name="ewald_step",
    )(*inputs, *[jnp.asarray(t) for t in tables])
    forces, energy = pl.pallas_call(
        put,
        out_shape=(
            jax.ShapeDtypeStruct((3, atoms), f32),
            jax.ShapeDtypeStruct((1, atoms), f32),
        ),
        in_specs=[vmem] * 2,
        out_specs=(anywhere, anywhere),
        scratch_shapes=[sems((2,))],
        compiler_params=pltpu.CompilerParams(vmem_limit_bytes=262144),
        name="put_results",
    )(forces, energy)
    return forces, energy[0]


def solution(mesh):
    plan = make_plan(mesh.shape["row"], mesh.shape["col"])
    placed = (
        P(("row", "col")),
        P(("row", "col")),
        P(("row", "col")),
        P(None, ("row", "col")),
        P(None, ("row", "col")),
        P("col", "row", None),
    )
    return jax.shard_map(
        body if plan is None else functools.partial(fast_body, plan),
        mesh=mesh,
        in_specs=placed,
        out_specs=(P(None, ("row", "col")), P(("row", "col"))),
        check_vma=False,
    )
```
